32 devices in a mesh: section: 2 (over core), row: 4 (over y, x), col: 4 (over z).
Axes of the slice: x: 2, y: 2, z: 4, core: 2. Of those that a mesh axis runs over, the one named last changes fastest.
Arguments:
- inputs: bfloat16 [2, 1536, 2048], P(None, 'col', 'row'), may hold values from -6 to 6
- lengths: int32 [2, 4, 3], P(None, 'col'), may hold values from 1 to 192, 384 in all within a row
- norm_gain: float32 [2, 2, 2048], P('section', None, 'row'), may hold values from 0.5 to 1.5
- norm_bias: float32 [2, 2, 2048], P('section', None, 'row'), may hold values from -3 to 3
- w_qkv: bfloat16 [2, 2048, 3, 2048], P('section', 'col', None, 'row'), may hold values from -0.125 to 0.125
- b_qkv: float32 [2, 3, 2048], P('section', None, 'row'), may hold values from -3 to 3
- w_out: bfloat16 [2, 2048, 2048], P('section', 'row', 'col'), may hold values from -0.5 to 0.5
- w_gate_up: bfloat16 [2, 2048, 2, 5632], P('section', 'col', None, 'row'), may hold values from -0.125 to 0.125
- w_down: bfloat16 [2, 5632, 2048], P('section', 'row', 'col'), may hold values from -0.078125 to 0.078125
- grad_out: bfloat16 [2, 1536, 2048], P(None, 'col', 'row'), may hold values from -6 to 6
Outputs:
- activations: bfloat16 [2, 2, 1536, 2048], P('section', None, 'col', 'row')
- input_grad: bfloat16 [2, 2, 1536, 2048], P('section', None, 'col', 'row')
- grad_norm_gain: float32 [2, 2, 2048], P('section', None, 'row')
- grad_norm_bias: float32 [2, 2, 2048], P('section', None, 'row')
- grad_w_qkv: float32 [2, 2048, 3, 2048], P('section', 'col', None, 'row')
- grad_b_qkv: float32 [2, 3, 2048], P('section', None, 'row')
- grad_w_out: float32 [2, 2048, 2048], P('section', 'row', 'col')
- grad_w_gate_up: float32 [2, 2048, 2, 5632], P('section', 'col', None, 'row')
- grad_w_down: float32 [2, 5632, 2048], P('section', 'row', 'col')
The draws below stay inside these ranges and needn't reach their ends.
Inputs may be any that keep to these rules, and one draw needn't show every extreme that they name: `lengths`: each block of 384 tokens of a micro-batch holds 3 whole sequences that fill it; the longest in every block has exactly 192 tokens.
All inputs are finite; a program needn't handle non-finite values.
Results may differ from the reference program's by a relative error of at most 0.017.
Values may be sent and summed in bfloat16 or wider, within the bound.
A program may use at most 256 MiB of HBM per device.

```python
import math
import jax
import jax.numpy as jnp
import numpy as np
from jax import lax

D = 2048
HEADS = 32
HEAD_DIM = 64
FF = 5632
ROT = 16
TOK_DEV = 384
MICRO = 2
SEGS = 3
TOKENS = 1536
N_COL = 4


def block_levels(stream_key, shape, cuts, least, largest):
    def one(dim, shards_of):
        draws = jax.random.uniform(jax.random.fold_in(jax.random.fold_in(stream_key, 6), dim), (shards_of,), jnp.float32, least / len(cuts), largest / len(cuts))
        return jnp.repeat(jnp.exp(draws), shape[dim] // shards_of).reshape((-1,) + (1,) * (len(shape) - dim - 1))

    level = one(*cuts[0])
    for cut in cuts[1:]:
        level = level * one(*cut)
    return level


def length_profile(count, total, reach, slope):
    weights = [(1 << 20) // math.isqrt(rank ** slope) + 1 for rank in range(2, count + 1)]
    rest, given = total - reach - (count - 1), [1] * (count - 1)
    while rest > 0:
        movable = [i for i in range(count - 1) if given[i] < reach]
        pool, budget = sum([weights[i] for i in movable]), rest
        for i in movable:
            addition = min(reach - given[i], max(1, budget * weights[i] // pool), rest)
            given[i] = given[i] + addition
            rest = rest - addition
    return np.array([reach] + given)


def uneven_parts(key, count, total, reach, lean):
    if count == 2:
        one = jax.random.randint(key, (), max(1, total - reach), min(reach, total - 1) + 1)
        return jnp.stack([one, total - one])
    tallies = jnp.asarray(length_profile(count, total, reach, lean), jnp.int32)
    pairs = (count - 1) // 2
    donor, receiver = tallies[1:1 + 2 * pairs:2], tallies[2:2 + 2 * pairs:2]
    margin = jnp.minimum(donor - 1, reach - receiver)
    moved = jax.random.randint(jax.random.fold_in(key, 1), (pairs,), 0, 1 << 20) % (margin + 1)
    tallies = tallies.at[1:1 + 2 * pairs:2].set(donor - moved).at[2:2 + 2 * pairs:2].set(receiver + moved)
    return tallies[jax.random.permutation(jax.random.fold_in(key, 2), count)]


def normal_values(stream_key, extent, scale, most, cuts=(), kind=jnp.bfloat16):
    drawn = scale * jax.random.normal(stream_key, extent, jnp.float32)
    if cuts:
        drawn = drawn * block_levels(stream_key, extent, cuts, -0.22, 0.18)
    return jnp.clip(drawn, -most, most).astype(kind)


def setup_inputs(seed: int = 0) -> dict:
    key_of = jax.random.split(jax.random.key(seed), 11)
    return {
        "inputs": normal_values(key_of[0], (MICRO, TOKENS, D), 1.0, 6.0, ((1, 4), (2, 4))),
        "lengths": jax.vmap(lambda own: uneven_parts(own, SEGS, TOK_DEV, TOK_DEV // 2, 1))(jax.random.split(key_of[1], MICRO * N_COL)).reshape((MICRO, N_COL, SEGS)).astype(jnp.int32),
        "norm_gain": jnp.clip(1.0 + 0.1 * jax.random.normal(key_of[2], (2, 2, D), jnp.float32), 0.5, 1.5),
        "norm_bias": normal_values(key_of[3], (2, 2, D), 0.5, 3.0, ((0, 2), (2, 4)), jnp.float32),
        "w_qkv": normal_values(key_of[4], (2, D, 3, D), D ** -0.5, 0.125, ((0, 2), (1, 4), (3, 4))),
        "b_qkv": normal_values(key_of[5], (2, 3, D), 0.5, 3.0, ((0, 2), (2, 4)), jnp.float32),
        "w_out": normal_values(key_of[6], (2, D, D), (D // 16) ** -0.5, 0.5, ((0, 2), (1, 4), (2, 4))),
        "w_gate_up": normal_values(key_of[7], (2, D, 2, FF), D ** -0.5, 0.125, ((0, 2), (1, 4), (3, 4))),
        "w_down": normal_values(key_of[8], (2, FF, D), FF ** -0.5, 0.078125, ((0, 2), (1, 4), (2, 4))),
        "grad_out": normal_values(key_of[9], (MICRO, TOKENS, D), 1.0, 6.0, ((1, 4), (2, 4))),
    }


PRECISE = lax.Precision.HIGHEST
EPSILON = 1e-05

@jax.custom_vjp
def low(v):
    return lax.optimization_barrier(v.astype(jnp.bfloat16)).astype(jnp.float32)

@jax.custom_vjp
def low_back(v):
    return v

def low_keep(v):
    return (low(v), None)

def low_pass(kept, grad):
    return (grad,)

def back_keep(v):
    return (v, None)

def back_low(kept, grad):
    return (low(grad),)
low.defvjp(low_keep, low_pass)
low_back.defvjp(back_keep, back_low)

def layout(seq_lengths):
    seq_lengths = seq_lengths.astype(jnp.int32)
    end_points = jnp.cumsum(seq_lengths).astype(jnp.int32)
    places = jnp.arange(TOK_DEV, dtype=jnp.int32)
    passed = places[:, None] >= end_points[None, :]
    segment = lax.optimization_barrier(jnp.sum(passed.astype(jnp.int32), axis=1)).astype(jnp.int32)
    starts = lax.optimization_barrier(jnp.sum(jnp.where(passed, seq_lengths[None, :], 0), axis=1)).astype(jnp.int32)
    offset = (places - starts).astype(jnp.float32)
    allowed = (segment[:, None] == segment[None, :]) & (places[None, :] <= places[:, None])
    frequency = 10000.0 ** (-(jnp.arange(ROT // 2, dtype=jnp.float32) * 2.0 / ROT))
    angles = offset[:, None] * frequency[None, :]
    return (allowed, jnp.cos(angles), jnp.sin(angles))

def rotate(values, cosine, sine_table):
    halfway = ROT // 2
    leading = values[..., :halfway]
    trailing = values[..., halfway:ROT]
    cosine = cosine[:, None, :]
    sine_table = sine_table[:, None, :]
    return jnp.concatenate([leading * cosine - trailing * sine_table, trailing * cosine + leading * sine_table, values[..., ROT:]], axis=-1)

def norm_rows(values, gain_row, shift_row):
    centre = lax.optimization_barrier(jnp.mean(values, axis=-1, keepdims=True))
    spread = lax.optimization_barrier(jnp.mean(values * values, axis=-1, keepdims=True)) - centre * centre
    return (values - centre) * lax.rsqrt(spread + EPSILON) * gain_row + shift_row

def attend_block(pieces):
    queries, keys_in, values, seq_lengths = pieces
    allowed, cosine, sine_table = layout(seq_lengths)
    scaling = 1.0 / math.sqrt(HEAD_DIM)
    queries = low(rotate(queries, cosine, sine_table))
    keys_in = low(rotate(keys_in, cosine, sine_table))
    values = low(values)
    scores = low_back(jnp.einsum('qhd,khd->hqk', queries, keys_in, precision=PRECISE) * scaling)
    scores = jnp.where(allowed[None], scores, -1e+30)
    totals = jnp.log(lax.optimization_barrier(jnp.sum(jnp.exp(scores), axis=-1, keepdims=True)))
    soft_weights = low(jnp.exp(scores - totals))
    return jnp.einsum('hqk,khd->qhd', soft_weights, values, precision=PRECISE)

def layer(layer_in, seq_lengths, layer_params):
    gain_rows, shifts, w_qkv, b_qkv, w_out, w_gate_up, w_down = layer_params
    normed_one = low(norm_rows(layer_in, gain_rows[0], shifts[0]))
    mixed_rows = low_back(jnp.einsum('td,dkh->tkh', normed_one, w_qkv, precision=PRECISE) + b_qkv[None])
    shaped = mixed_rows.reshape(N_COL, TOK_DEV, 3, HEADS, HEAD_DIM)
    attended = lax.map(jax.checkpoint(attend_block), (shaped[:, :, 0], shaped[:, :, 1], shaped[:, :, 2], seq_lengths))
    attended = low_back(low(attended.reshape(TOKENS, D)))
    branch = low_back(jnp.dot(attended, w_out, precision=PRECISE))
    hidden_state = layer_in + branch
    normed_two = low(norm_rows(hidden_state, gain_rows[1], shifts[1]))
    gate_up = low_back(jnp.einsum('td,dkf->tkf', normed_two, w_gate_up, precision=PRECISE))
    activated = low(jax.nn.silu(gate_up[:, 0]) * gate_up[:, 1])
    return hidden_state + low_back(jnp.dot(activated, w_down, precision=PRECISE))

def reference(inputs, lengths, norm_gain, norm_bias, w_qkv, b_qkv, w_out, w_gate_up, w_down, grad_out):

    def section_params(section_index):
        return tuple((array_in[section_index].astype(jnp.float32) for array_in in (norm_gain, norm_bias, w_qkv, b_qkv, w_out, w_gate_up, w_down)))
    first_params = section_params(0)
    second_params = section_params(1)
    first_totals = jax.tree.map(jnp.zeros_like, first_params)
    second_totals = jax.tree.map(jnp.zeros_like, second_params)
    first_outs, second_outs, first_grads, second_grads = ([], [], [], [])
    for micro_index in range(MICRO):
        seq_lengths = lengths[micro_index]
        middle, pull_first = jax.vjp(lambda layer_in, layer_params: layer(layer_in, seq_lengths, layer_params), inputs[micro_index].astype(jnp.float32), first_params)
        middle_sent = middle.astype(jnp.bfloat16)
        section_out, pull_second = jax.vjp(lambda layer_in, layer_params: layer(layer_in, seq_lengths, layer_params), middle_sent.astype(jnp.float32), second_params)
        back_in, back_second = pull_second(grad_out[micro_index].astype(jnp.float32))
        back_sent = back_in.astype(jnp.bfloat16)
        back_input, back_first = pull_first(back_sent.astype(jnp.float32))
        first_totals = jax.tree.map(jnp.add, first_totals, back_first)
        second_totals = jax.tree.map(jnp.add, second_totals, back_second)
        first_outs.append(middle_sent)
        second_outs.append(section_out.astype(jnp.bfloat16))
        first_grads.append(back_input.astype(jnp.bfloat16))
        second_grads.append(back_sent)
    activations = jnp.stack([jnp.stack(first_outs), jnp.stack(second_outs)])
    input_grad = jnp.stack([jnp.stack(first_grads), jnp.stack(second_grads)])
    stacked = [jnp.stack([first_totals[index], second_totals[index]]) for index in range(7)]
    return (activations, input_grad, stacked[0], stacked[1], stacked[2], stacked[3], stacked[4], stacked[5], stacked[6])
```

```python
import math

import jax
import jax.numpy as jnp
from jax import lax
from jax.sharding import PartitionSpec as P

HEAD_DIM = 64
ROT = 16
TOK_DEV = 384
MICRO = 2
EPSILON = 1e-05
AXES = ("section", "row", "col")
BF16 = jnp.bfloat16
F32 = jnp.float32


def dot(left, right, left_dim, right_dim):
    return lax.dot_general(
        left, right, (((left_dim,), (right_dim,)), ((), ())), preferred_element_type=F32
    )


class Grid:
    def __init__(self):
        self.rows = lax.axis_size("row")
        self.cols = lax.axis_size("col")
        self.half = self.cols // 2
        self.s = lax.axis_index("section")
        self.r = lax.axis_index("row")
        self.c = lax.axis_index("col")
        self.g = self.c // self.half
        self.folded = jnp.where(self.s == 0, self.c, self.cols - 1 - self.c)
        self.is_chain = self.s == self.g

    def flat(self, s, r, c):
        return (s * self.rows + r) * self.cols + c

    def everywhere(self, moves):
        return [
            (self.flat(s0, r, c0), self.flat(s1, r, c1))
            for r in range(self.rows)
            for (s0, c0, s1, c1) in moves
        ]

    def send(self, value, moves):
        return lax.ppermute(value, AXES, self.everywhere(moves))

    def chain(self, value, hops):
        last = self.cols - 1
        moves = [(0, a, 0, b) for a, b in hops] + [(1, last - a, 1, last - b) for a, b in hops]
        return self.send(value, moves)

    def to_partner_core(self, value):
        moves = [(c // self.half, c, 1 - c // self.half, c) for c in range(self.cols)]
        return self.send(value, moves)

    def from_chain_partner(self, value):
        moves = [(1 - c // self.half, c, c // self.half, c) for c in range(self.cols)]
        return self.send(value, moves)

    def scatter_blocks(self, first, second):
        moves = [
            (g, b, b % 2, g * self.half + b // 2) for g in range(2) for b in range(self.cols)
        ]
        return self.send(jnp.where(self.s == 0, first, second), moves)

    def return_blocks(self, value):
        moves = [
            (b % 2, g * self.half + b // 2, g, b) for g in range(2) for b in range(self.cols)
        ]
        return self.send(value, moves)

    def hand_on(self, value, forward):
        moves = []
        for s in range(2):
            for c in range(self.half):
                a, b = (c, c + self.half) if forward else (c + self.half, c)
                moves.append((s, a, s, b))
        return self.send(value, moves)

    def gather_shards(self, own):
        cols, half = self.cols, self.half
        left, right = [own], [own]
        shards = [own]
        for k in range(1, cols):
            lefts = [(u + 1, u) for u in range(cols - k)]
            if k <= half:
                got = self.chain(left[-1], lefts)
                left.append(got)
                shards.append(got)
                continue
            shards.append(None)
            left.append(left[-1] if k == half + 1 and half == 2 else self.chain(left[-1], lefts))
        if half == 2:
            got = self.chain(jnp.where(self.folded == 0, own, left[2]), [(1, 0), (0, 1)])
            shards[3] = got
        else:
            for j in range(1, half):
                got = self.chain(right[-1], [(u, u + 1) for u in range(j - 1, half - 1)])
                right.append(got)
                k = cols - j
                shards[k] = jnp.where(self.folded + k < cols, left[k], got)
        result = []
        for shard in shards:
            other = self.to_partner_core(shard)
            result.append(jnp.where(self.is_chain, shard, other))
        return result

    def scatter_grads(self, parts):
        cols, half = self.cols, self.half
        mine = []
        for part in parts:
            other = self.from_chain_partner(part.astype(BF16))
            total = part + other.astype(F32)
            mine.append(jnp.where(self.is_chain, total, 0.0))
        in_group = self.folded < half
        if half == 2:
            got = self.chain(mine[3].astype(BF16), [(0, 1), (1, 0)]).astype(F32)
            at_zero = jnp.where(self.folded == 0, got, 0.0)
            carry = jnp.where(self.folded == 0, 0.0, got)
            for t in range(2, cols):
                payload = (carry + mine[cols - t]).astype(BF16)
                carry = self.chain(payload, [(u, u + 1) for u in range(t)]).astype(F32)
            return mine[0] + carry + at_zero
        carry = jnp.zeros_like(mine[0])
        for t in range(1, cols):
            payload = (carry + mine[cols - t]).astype(BF16)
            carry = self.chain(payload, [(u, u + 1) for u in range(t)]).astype(F32)
        back = jnp.zeros_like(mine[0])
        for t in range(1, half):
            payload = (back + mine[cols - half + t]).astype(BF16)
            hops = [(u, u - 1) for u in range(half - t, half)]
            back = self.chain(payload, hops).astype(F32)
        return mine[0] + carry + back

    def column_block(self, k):
        step = jnp.where(self.g == 0, k, self.cols - k)
        return lax.rem(self.c + step, self.cols)

    def rotate_row(self, value, d):
        return lax.ppermute(
            value, "row", [(r, (r + d) % self.rows) for r in range(self.rows)]
        )

    def row_gather(self, block):
        width = block.shape[1]
        full = jnp.zeros((block.shape[0], width * self.rows), block.dtype)
        for d in range(self.rows):
            got = block if d == 0 else self.rotate_row(block, d)
            owner = lax.rem(self.r + self.rows - d, self.rows)
            full = lax.dynamic_update_slice(full, got, (0, owner * width))
        return full

    def row_scatter(self, partial):
        width = partial.shape[1] // self.rows
        total = None
        for d in range(self.rows):
            target = lax.rem(self.r + d, self.rows)
            piece = lax.dynamic_slice(partial, (0, target * width), (partial.shape[0], width))
            got = piece if d == 0 else self.rotate_row(piece.astype(BF16), d).astype(F32)
            total = got if total is None else total + got
        return total

    def to_chunks(self, full):
        width = full.shape[1] // self.cols
        return jnp.concatenate(
            [
                lax.dynamic_slice(
                    full, (0, self.column_block(k) * width), (full.shape[0], width)
                )
                for k in range(self.cols)
            ],
            axis=1,
        )

    def from_chunks(self, chunked):
        width = chunked.shape[1] // self.cols
        full = jnp.zeros_like(chunked)
        for k in range(self.cols):
            piece = chunked[:, k * width : (k + 1) * width]
            full = lax.dynamic_update_slice(full, piece, (0, self.column_block(k) * width))
        return full


def layout(seq_lengths):
    end_points = jnp.cumsum(seq_lengths)
    places = jnp.arange(TOK_DEV, dtype=jnp.int32)
    passed = places[:, None] >= end_points[None, :]
    segment = jnp.sum(passed.astype(jnp.int32), axis=1)
    starts = jnp.sum(jnp.where(passed, seq_lengths[None, :], 0), axis=1)
    offset = (places - starts).astype(F32)
    allowed = (segment[:, None] == segment[None, :]) & (places[None, :] <= places[:, None])
    frequency = 10000.0 ** (-(jnp.arange(ROT // 2, dtype=F32) * 2.0 / ROT))
    angles = offset[:, None] * frequency[None, :]
    return (allowed, jnp.cos(angles), jnp.sin(angles))


def rotate(values, cosine, sine_table):
    halfway = ROT // 2
    leading = values[..., :halfway]
    trailing = values[..., halfway:ROT]
    cosine = cosine[:, None, :]
    sine_table = sine_table[:, None, :]
    return jnp.concatenate(
        [
            leading * cosine - trailing * sine_table,
            trailing * cosine + leading * sine_table,
            values[..., ROT:],
        ],
        axis=-1,
    )


def unit_rows(full):
    rows = full.astype(F32)
    centre = jnp.mean(rows, axis=-1, keepdims=True)
    spread = jnp.mean(rows * rows, axis=-1, keepdims=True) - centre * centre
    scaled = lax.rsqrt(spread + EPSILON)
    return (rows - centre) * scaled, scaled


def masked_scores(queries, keys_in, allowed, scaling):
    scores = jnp.einsum("qhd,khd->hqk", queries, keys_in, preferred_element_type=F32) * scaling
    return jnp.where(allowed[None], scores, -1e30)


def attention(mixed, tables, scaling):
    allowed, cosine, sine_table = tables
    rows = mixed[0].shape[0]
    shaped = [part.reshape(rows, -1, HEAD_DIM) for part in mixed]
    queries = rotate(shaped[0], cosine, sine_table).astype(BF16)
    keys_in = rotate(shaped[1], cosine, sine_table).astype(BF16)
    values = shaped[2].astype(BF16)
    scores = masked_scores(queries, keys_in, allowed, scaling)
    totals = jnp.log(jnp.sum(jnp.exp(scores), axis=-1, keepdims=True))
    soft_weights = jnp.exp(scores - totals).astype(BF16)
    attended = jnp.einsum("hqk,khd->qhd", soft_weights, values, preferred_element_type=F32)
    return attended.astype(BF16).reshape(rows, -1), (queries, keys_in, values, totals)


def attention_back(grad_attended, saved, tables, scaling):
    allowed, cosine, sine_table = tables
    queries, keys_in, values, totals = saved
    rows = grad_attended.shape[0]
    grad_heads = grad_attended.reshape(rows, -1, HEAD_DIM)
    soft_weights = jnp.exp(masked_scores(queries, keys_in, allowed, scaling) - totals)
    grad_values = jnp.einsum(
        "hqk,qhd->khd", soft_weights.astype(BF16), grad_heads, preferred_element_type=F32
    )
    grad_soft = jnp.einsum("qhd,khd->hqk", grad_heads, values, preferred_element_type=F32)
    grad_scores = (
        soft_weights * (grad_soft - jnp.sum(soft_weights * grad_soft, axis=-1, keepdims=True))
    ).astype(BF16)
    grad_queries = (
        jnp.einsum("hqk,khd->qhd", grad_scores, keys_in, preferred_element_type=F32) * scaling
    )
    grad_keys = (
        jnp.einsum("hqk,qhd->khd", grad_scores, queries, preferred_element_type=F32) * scaling
    )
    return [
        part.astype(BF16).reshape(rows, -1)
        for part in (
            rotate(grad_queries, cosine, -sine_table),
            rotate(grad_keys, cosine, -sine_table),
            grad_values,
        )
    ]


def forward_block(grid, block, tables, small, weights, scaling):
    gains, shifts, bias = small
    w_qkv, w_out, w_gate_up, w_down = weights
    unit_one, scaled_one = unit_rows(grid.row_gather(block))
    normed_one = grid.to_chunks((unit_one * gains[0] + shifts[0]).astype(BF16))
    mixed = [dot(normed_one, w_qkv[i], 1, 0) + bias[i] for i in range(3)]
    attended, kept = attention(mixed, tables, scaling)
    branch = grid.row_scatter(grid.from_chunks(dot(attended, w_out, 1, 0)))
    hidden = block.astype(F32) + branch
    unit_two, scaled_two = unit_rows(grid.row_gather(hidden.astype(BF16)))
    normed_two = grid.to_chunks((unit_two * gains[1] + shifts[1]).astype(BF16))
    gate = dot(normed_two, w_gate_up[0], 1, 0)
    up = dot(normed_two, w_gate_up[1], 1, 0)
    activated = (jax.nn.silu(gate) * up).astype(BF16)
    output = hidden + grid.row_scatter(grid.from_chunks(dot(activated, w_down, 1, 0)))
    saved = (
        normed_one,
        unit_one,
        scaled_one,
        kept,
        attended,
        normed_two,
        unit_two,
        scaled_two,
        gate,
        up,
        activated,
    )
    return output.astype(BF16), saved


def norm_back(grid, partial, unit_full, scaled, gain):
    weighted = partial * gain
    sums = lax.psum(
        jnp.stack([jnp.sum(weighted, axis=-1), jnp.sum(weighted * unit_full, axis=-1)]), "row"
    )
    grad_normed = grid.row_scatter(partial)
    rows, width = grad_normed.shape
    features = unit_full.shape[1]
    unit = lax.dynamic_slice(unit_full, (0, grid.r * width), (rows, width))
    gain_here = lax.dynamic_slice(gain, (grid.r * width,), (width,))
    grad_values = scaled * (
        grad_normed * gain_here
        - sums[0][:, None] / features
        - unit * (sums[1][:, None] / features)
    )
    return grad_values, jnp.sum(grad_normed * unit, axis=0), jnp.sum(grad_normed, axis=0)


def backward_block(grid, grad_output, saved, tables, small, weights, scaling):
    (
        normed_one,
        unit_one,
        scaled_one,
        kept,
        attended,
        normed_two,
        unit_two,
        scaled_two,
        gate,
        up,
        activated,
    ) = saved
    gains = small[0]
    w_qkv, w_out, w_gate_up, w_down = weights
    grad_down_in = grid.to_chunks(grid.row_gather(grad_output))
    grad_act = dot(grad_down_in, w_down, 1, 1)
    sigmoid = jax.nn.sigmoid(gate)
    grad_gate = (grad_act * up * sigmoid * (1.0 + gate * (1.0 - sigmoid))).astype(BF16)
    grad_up = (grad_act * (gate * sigmoid)).astype(BF16)
    grad_normed_two = dot(grad_gate, w_gate_up[0], 1, 1) + dot(grad_up, w_gate_up[1], 1, 1)
    grad_hidden, gain_two, shift_two = norm_back(
        grid, grid.from_chunks(grad_normed_two), unit_two, scaled_two, gains[1]
    )
    grad_hidden = grad_output.astype(F32) + grad_hidden
    grad_out_in = grid.to_chunks(grid.row_gather(grad_hidden.astype(BF16)))
    grad_attended = dot(grad_out_in, w_out, 1, 1).astype(BF16)
    grad_mixed = attention_back(grad_attended, kept, tables, scaling)
    grad_normed_one = sum(dot(grad_mixed[i], w_qkv[i], 1, 1) for i in range(3))
    grad_input, gain_one, shift_one = norm_back(
        grid, grid.from_chunks(grad_normed_one), unit_one, scaled_one, gains[0]
    )
    grad_input = grad_hidden + grad_input
    grad_bias = jnp.stack([jnp.sum(part.astype(F32), axis=0) for part in grad_mixed])
    small_terms = jnp.concatenate(
        [jnp.stack([gain_one, gain_two, shift_one, shift_two]), grad_bias]
    )
    pairs = (
        (normed_one, grad_mixed[0]),
        (normed_one, grad_mixed[1]),
        (normed_one, grad_mixed[2]),
        (attended, grad_out_in),
        (normed_two, grad_gate),
        (normed_two, grad_up),
        (activated, grad_down_in),
    )
    return grad_input.astype(BF16), small_terms, pairs


def weight_grads(grid, pairs):
    joined = [
        tuple(jnp.concatenate([pairs[m][i][side] for m in range(MICRO)]) for side in range(2))
        for i in range(7)
    ]
    width = joined[0][0].shape[1] // grid.cols

    def by_rows(indices):
        return [
            jnp.stack(
                [
                    dot(joined[i][0][:, k * width : (k + 1) * width], joined[i][1], 0, 0)
                    for i in indices
                ]
            )
            for k in range(grid.cols)
        ]

    def by_columns(i):
        return [
            dot(joined[i][0], joined[i][1][:, k * width : (k + 1) * width], 0, 0)
            for k in range(grid.cols)
        ]

    return by_rows((0, 1, 2)), by_columns(3), by_rows((4, 5)), by_columns(6)


def on_device(
    inputs, lengths, norm_gain, norm_bias, w_qkv, b_qkv, w_out, w_gate_up, w_down, grad_out
):
    grid = Grid()
    scaling = 1.0 / math.sqrt(HEAD_DIM)
    start = grid.scatter_blocks(inputs, grad_out)
    own_lengths = grid.scatter_blocks(lengths, lengths)[:, 0]
    tables = [layout(own_lengths[m]) for m in range(MICRO)]

    packed = jnp.concatenate([norm_gain[0], norm_bias[0], b_qkv[0]])
    everyones = lax.all_gather(packed, ("section", "row"))
    everyones = everyones.reshape(2, grid.rows, 7, packed.shape[1])
    ours = lax.dynamic_index_in_dim(everyones, grid.g, 0, keepdims=False)
    gains = [ours[:, i].reshape(-1) for i in range(2)]
    shifts = [ours[:, 2 + i].reshape(-1) for i in range(2)]
    bias = lax.dynamic_index_in_dim(ours, grid.r, 0, keepdims=False)[4:]
    small = (gains, shifts, bias)

    weights = (
        jnp.concatenate(grid.gather_shards(jnp.swapaxes(w_qkv[0], 0, 1)), axis=1),
        jnp.concatenate(grid.gather_shards(w_out[0]), axis=1),
        jnp.concatenate(grid.gather_shards(jnp.swapaxes(w_gate_up[0], 0, 1)), axis=1),
        jnp.concatenate(grid.gather_shards(w_down[0]), axis=1),
    )

    def forward(blocks):
        results = [
            forward_block(grid, blocks[m], tables[m], small, weights, scaling)
            for m in range(MICRO)
        ]
        return jnp.stack([result[0] for result in results]), [result[1] for result in results]

    def backward(grads, saved):
        results = [
            backward_block(grid, grads[m], saved[m], tables[m], small, weights, scaling)
            for m in range(MICRO)
        ]
        return (
            jnp.stack([result[0] for result in results]),
            sum(result[1] for result in results),
            weight_grads(grid, [result[2] for result in results]),
        )

    is_first = grid.g == 0
    out_first, saved_first = forward(start)
    out_second, saved_second = forward(grid.hand_on(out_first, True))
    activations = grid.return_blocks(jnp.where(is_first, out_first, out_second))
    grad_second, small_second, large_second = backward(start, saved_second)
    grad_first, small_first, large_first = backward(grid.hand_on(grad_second, False), saved_first)
    input_grad = grid.return_blocks(jnp.where(is_first, grad_first, grad_second))

    large = jax.tree.map(
        lambda first, second: jnp.where(is_first, first, second), large_first, large_second
    )
    part_qkv, part_out, part_gate_up, part_down = [grid.scatter_grads(parts) for parts in large]
    small_total = jnp.where(is_first, small_first, small_second)
    slots = jnp.stack(
        [jnp.where(is_first, small_total, 0.0), jnp.where(is_first, 0.0, small_total)]
    )
    slots = lax.psum(slots, ("section", "col"))
    sums = lax.dynamic_index_in_dim(slots, grid.s, 0, keepdims=False)
    return (
        activations[None],
        input_grad[None],
        sums[None, 0:2],
        sums[None, 2:4],
        jnp.swapaxes(part_qkv, 0, 1)[None],
        sums[None, 4:7],
        part_out[None],
        jnp.swapaxes(part_gate_up, 0, 1)[None],
        part_down[None],
    )


def solution(mesh):
    in_specs = (
        P(None, "col", "row"),
        P(None, "col", None),
        P("section", None, "row"),
        P("section", None, "row"),
        P("section", "col", None, "row"),
        P("section", None, "row"),
        P("section", "row", "col"),
        P("section", "col", None, "row"),
        P("section", "row", "col"),
        P(None, "col", "row"),
    )
    out_specs = (
        P("section", None, "col", "row"),
        P("section", None, "col", "row"),
        P("section", None, "row"),
        P("section", None, "row"),
        P("section", "col", None, "row"),
        P("section", None, "row"),
        P("section", "row", "col"),
        P("section", "col", None, "row"),
        P("section", "row", "col"),
    )
    return jax.shard_map(
        on_device, mesh=mesh, in_specs=in_specs, out_specs=out_specs, check_vma=False
    )
```

```python
import functools
import math

import jax
import jax.numpy as jnp
from jax import lax
from jax.experimental import pallas as pl
from jax.experimental.pallas import tpu as pltpu
from jax.sharding import Mesh
from jax.sharding import PartitionSpec as P

HEAD_DIM = 64
ROT = 16
TOK_DEV = 384
MICRO = 2
EPSILON = 1e-05
LANES = 128
WIDE = 256
AXES = ("section", "row", "half", "pair")
BF16 = jnp.bfloat16
F32 = jnp.float32
MESH = pl.DeviceIdType.MESH
VMEM = pl.BlockSpec(memory_space=pltpu.VMEM)
HBM = pl.BlockSpec(memory_space=pl.ANY)


def dot(left, right, left_dim, right_dim):
    return lax.dot_general(
        left, right, (((left_dim,), (right_dim,)), ((), ())), preferred_element_type=F32
    )


def block_of(k, pairs):
    half = lax.rem(lax.axis_index("section") + k // pairs, 2)
    return half * pairs + lax.rem(lax.axis_index("pair") + k % pairs, pairs)


def tiles(width, tile=WIDE):
    return [(start, min(tile, width - start)) for start in range(0, width, tile)]


def peer_of(r, d):
    return lax.rem(r // 2 + d // 2, 2) * 2 + lax.rem(lax.rem(r, 2) + d % 2, 2)


ROWS = 4
OTHERS = (3, 1, 2)


def row_barrier(r):
    barrier = pltpu.get_barrier_semaphore()
    for d in OTHERS:
        pl.semaphore_signal(
            barrier, inc=1, device_id={"row": peer_of(r, d)}, device_id_type=MESH
        )
    pl.semaphore_wait(barrier, ROWS - 1)


def remote(source, target, send_sem, recv_sem, peer):
    return pltpu.make_async_remote_copy(
        src_ref=source,
        dst_ref=target,
        send_sem=send_sem,
        recv_sem=recv_sem,
        device_id={"row": peer},
        device_id_type=MESH,
    )


def layer_norm(full_ref, out_ref, mean_ref, rstd_ref, gain_of, shift_of, first, rows):
    step = 32
    count = full_ref.shape[0] * full_ref.shape[2]

    @pl.loop(0, rows // step)
    def _(i):
        at = pl.ds(pl.multiple_of(first + i * step, step), step)
        total = jnp.zeros((step, 1), F32)
        square = jnp.zeros((step, 1), F32)
        for b in range(full_ref.shape[0]):
            block = full_ref[b, at, :].astype(F32)
            total = total + jnp.sum(block, axis=-1, keepdims=True)
            square = square + jnp.sum(block * block, axis=-1, keepdims=True)
        mean = total / count
        rstd = lax.rsqrt(square / count - mean * mean + EPSILON)
        mean_ref[at, :] = mean
        rstd_ref[at, :] = rstd
        for b in range(full_ref.shape[0]):
            unit = (full_ref[b, at, :].astype(F32) - mean) * rstd
            out_ref[b, at, :] = (unit * gain_of(b) + shift_of(b)).astype(BF16)


def rows_of(m):
    return pl.ds(m * TOK_DEV, TOK_DEV)


def gather_norm_kernel(
    x_ref, par_ref, full_ref, normed_ref, par_full_ref, mean_ref, rstd_ref, send, recv, psend, precv
):
    r = lax.axis_index("row")
    row_barrier(r)

    def par_copy(d):
        return remote(
            par_ref, par_full_ref.at[r], psend.at[d - 1], precv.at[d - 1], peer_of(r, d)
        )

    def copy(m, d):
        return remote(
            x_ref.at[rows_of(m)],
            full_ref.at[r, rows_of(m)],
            send.at[m, d - 1],
            recv.at[m, d - 1],
            peer_of(r, d),
        )

    for d in OTHERS:
        par_copy(d).start()
    for m in range(MICRO):
        for d in OTHERS:
            copy(m, d).start()
    full_ref[pl.ds(r, 1)] = x_ref[...][None]
    par_full_ref[pl.ds(r, 1)] = par_ref[...][None]
    for d in OTHERS:
        par_copy(d).wait()
    for m in range(MICRO):
        for d in OTHERS:
            copy(m, d).wait()
        layer_norm(
            full_ref,
            normed_ref,
            mean_ref,
            rstd_ref,
            lambda b: par_full_ref[b, 0:1, :],
            lambda b: par_full_ref[b, 2:3, :],
            m * TOK_DEV,
            TOK_DEV,
        )


def comm_params(collective_id):
    return pltpu.CompilerParams(collective_id=collective_id, has_side_effects=True)


def sems(*shape):
    return pltpu.SemaphoreType.DMA(shape)


def gather_norm(x, par):
    total, width = x.shape
    return pl.pallas_call(
        gather_norm_kernel,
        out_shape=(
            jax.ShapeDtypeStruct((ROWS, total, width), BF16),
            jax.ShapeDtypeStruct((ROWS, total, width), BF16),
            jax.ShapeDtypeStruct((ROWS,) + par.shape, F32),
            jax.ShapeDtypeStruct((total, 1), F32),
            jax.ShapeDtypeStruct((total, 1), F32),
        ),
        in_specs=[VMEM, VMEM],
        out_specs=(VMEM,) * 5,
        scratch_shapes=[sems(MICRO, 3), sems(MICRO, 3), sems(3), sems(3)],
        compiler_params=comm_params(0),
        name="gather_norm",
    )(x, par)


def gather_kernel(x_ref, full_ref, send, recv):
    r = lax.axis_index("row")
    row_barrier(r)

    def copy(d):
        return remote(x_ref, full_ref.at[r], send.at[d - 1], recv.at[d - 1], peer_of(r, d))

    for d in OTHERS:
        copy(d).start()
    full_ref[pl.ds(r, 1)] = x_ref[...][None]
    for d in OTHERS:
        copy(d).wait()


def gather(x):
    return pl.pallas_call(
        gather_kernel,
        out_shape=jax.ShapeDtypeStruct((ROWS,) + x.shape, BF16),
        in_specs=[VMEM],
        out_specs=VMEM,
        scratch_shapes=[sems(3), sems(3)],
        compiler_params=comm_params(1),
        name="row_gather",
    )(x)


def load_column_blocks(piece_refs, buffer, sem, width):
    pairs = len(piece_refs) // 2
    own = width // len(piece_refs)
    per_row = len(piece_refs) // ROWS
    copies = []
    for k, piece in enumerate(piece_refs):
        b = block_of(k, pairs)
        offset = pl.multiple_of(lax.rem(b, per_row) * own, own)
        copies.append(
            pltpu.make_async_copy(
                piece, buffer.at[b // per_row, :, pl.ds(offset, own)], sem.at[k]
            )
        )
    for copy in copies:
        copy.start()
    return copies


def load_row_blocks(piece_refs, buffer, sem, width):
    pairs = len(piece_refs) // 2
    own = width // len(piece_refs)
    per_row = len(piece_refs) // ROWS
    copies = []
    for k, piece in enumerate(piece_refs):
        b = block_of(k, pairs)
        offset = pl.multiple_of(lax.rem(b, per_row) * own, own)
        copies.append(
            pltpu.make_async_copy(
                piece, buffer.at[b // per_row, :, pl.ds(offset, own), :], sem.at[k]
            )
        )
    for copy in copies:
        copy.start()
    return copies


def exchange(r, partial, own_ref, send_buf, recv_buf, send, recv):
    def copy(m, d):
        return remote(
            send_buf.at[m, d - 1],
            recv_buf.at[m, d - 1],
            send.at[m, d - 1],
            recv.at[m, d - 1],
            peer_of(r, d),
        )

    width = own_ref.shape[1]
    for m in range(MICRO):
        for d in OTHERS + (0,):
            for start, size in tiles(width):
                cols = slice(start, start + size)
                part = partial(m, peer_of(r, d), cols)
                if d == 0:
                    own_ref[rows_of(m), cols] = part
                else:
                    send_buf[m, d - 1, :, cols] = part.astype(BF16)
            if d:
                copy(m, d).start()
    return copy


def out_norm_kernel(*refs):
    (att_ref, x_ref, par_full_ref), refs = refs[:3], refs[3:]
    pieces, refs = refs[:-13], refs[-13:]
    (hidden_ref, full_ref, normed_ref, mean_ref, rstd_ref) = refs[:5]
    (weight, send_buf, recv_buf, wsem, send, recv, gsend, grecv) = refs[5:]
    r = lax.axis_index("row")
    loads = load_column_blocks(pieces, weight, wsem, ROWS * hidden_ref.shape[1])
    row_barrier(r)
    for load in loads:
        load.wait()

    def partial(m, owner, cols):
        return dot(att_ref[rows_of(m), :], weight[owner, :, cols], 1, 0)

    copy = exchange(r, partial, hidden_ref, send_buf, recv_buf, send, recv)

    def spread(m, d):
        return remote(
            full_ref.at[r, rows_of(m)],
            full_ref.at[r, rows_of(m)],
            gsend.at[m, d - 1],
            grecv.at[m, d - 1],
            peer_of(r, d),
        )

    for m in range(MICRO):
        for d in OTHERS:
            copy(m, d).wait()
        step = 64

        @pl.loop(0, TOK_DEV // step)
        def _(i):
            here = pl.ds(pl.multiple_of(i * step, step), step)
            at = pl.ds(pl.multiple_of(m * TOK_DEV + i * step, step), step)
            hidden = hidden_ref[at, :] + x_ref[at, :].astype(F32)
            for d in OTHERS:
                hidden = hidden + recv_buf[m, d - 1, here, :].astype(F32)
            hidden_ref[at, :] = hidden
            full_ref[pl.ds(r, 1), at, :] = hidden.astype(BF16)[None]

        for d in OTHERS:
            spread(m, d).start()
    for m in range(MICRO):
        for d in OTHERS:
            spread(m, d).wait()
        layer_norm(
            full_ref,
            normed_ref,
            mean_ref,
            rstd_ref,
            lambda b: par_full_ref[b, 1:2, :],
            lambda b: par_full_ref[b, 3:4, :],
            m * TOK_DEV,
            TOK_DEV,
        )


def exchange_scratch(width):
    return [
        pltpu.VMEM((MICRO, 3, TOK_DEV, width), BF16),
        pltpu.VMEM((MICRO, 3, TOK_DEV, width), BF16),
    ]


def out_norm(attended, x, par_full, pieces):
    total, width = x.shape
    return pl.pallas_call(
        out_norm_kernel,
        out_shape=(
            jax.ShapeDtypeStruct((total, width), F32),
            jax.ShapeDtypeStruct((ROWS, total, width), BF16),
            jax.ShapeDtypeStruct((ROWS, total, width), BF16),
            jax.ShapeDtypeStruct((total, 1), F32),
            jax.ShapeDtypeStruct((total, 1), F32),
        ),
        in_specs=[VMEM] * 3 + [HBM] * len(pieces),
        out_specs=(VMEM,) * 5,
        scratch_shapes=[pltpu.VMEM((ROWS, attended.shape[1], width), BF16)]
        + exchange_scratch(width)
        + [
            sems(len(pieces)),
            sems(MICRO, 3),
            sems(MICRO, 3),
            sems(MICRO, 3),
            sems(MICRO, 3),
        ],
        compiler_params=comm_params(2),
        name="out_norm",
    )(attended, x, par_full, *pieces)


def down_kernel(*refs):
    (act_ref, hidden_ref), refs = refs[:2], refs[2:]
    pieces, refs = refs[:-8], refs[-8:]
    (out_ref, weight, total_ref, send_buf, recv_buf, wsem, send, recv) = refs
    r = lax.axis_index("row")
    loads = load_column_blocks(pieces, weight, wsem, ROWS * hidden_ref.shape[1])
    row_barrier(r)
    for load in loads:
        load.wait()

    def partial(m, owner, cols):
        return dot(act_ref[rows_of(m), :], weight[owner, :, cols], 1, 0)

    copy = exchange(r, partial, total_ref, send_buf, recv_buf, send, recv)
    for m in range(MICRO):
        for d in OTHERS:
            copy(m, d).wait()
        step = 64

        @pl.loop(0, TOK_DEV // step)
        def _(i):
            here = pl.ds(pl.multiple_of(i * step, step), step)
            at = pl.ds(pl.multiple_of(m * TOK_DEV + i * step, step), step)
            value = hidden_ref[at, :] + total_ref[at, :]
            for d in OTHERS:
                value = value + recv_buf[m, d - 1, here, :].astype(F32)
            out_ref[at, :] = value.astype(BF16)


def down(activated, hidden, pieces):
    total, width = hidden.shape
    return pl.pallas_call(
        down_kernel,
        out_shape=jax.ShapeDtypeStruct((total, width), BF16),
        in_specs=[VMEM] * 2 + [HBM] * len(pieces),
        out_specs=VMEM,
        scratch_shapes=[
            pltpu.VMEM((ROWS, activated.shape[1], width), BF16),
            pltpu.VMEM((total, width), F32),
        ]
        + exchange_scratch(width)
        + [sems(len(pieces)), sems(MICRO, 3), sems(MICRO, 3)],
        compiler_params=comm_params(3),
        name="down",
    )(activated, hidden, *pieces)


def back_kernel(n, spread_it, *refs):
    grads, refs = refs[:n], refs[n:]
    (base_ref, mean_ref, rstd_ref, gain_ref, resid_ref), refs = refs[:5], refs[5:]
    tail = 15 if spread_it else 12
    pieces, refs = refs[:-tail], refs[-tail:]
    if spread_it:
        (out_ref, full_ref, small_ref), refs = refs[:3], refs[3:]
        gsend, grecv = refs[-2:]
        refs = refs[:-2]
    else:
        (out_ref, small_ref), refs = refs[:2], refs[2:]
    (weight, total_ref, send_buf, recv_buf, stat_send, stat_recv, wsem, send, recv, ssem) = refs
    r = lax.axis_index("row")
    width = base_ref.shape[1]
    features = ROWS * width
    loads = load_row_blocks(pieces, weight, wsem, features)
    row_barrier(r)
    for load in loads:
        load.wait()

    def partial(m, owner, cols):
        return sum(
            dot(grads[i][rows_of(m), :], weight[owner, i, cols, :], 1, 1) for i in range(n)
        )

    copy = exchange(r, partial, total_ref, send_buf, recv_buf, send, recv)

    def stat_copy(m, d):
        return remote(
            stat_send.at[m],
            stat_recv.at[m, d - 1],
            ssem.at[0, m, d - 1],
            ssem.at[1, m, d - 1],
            peer_of(r, d),
        )

    step = 64
    gain = gain_ref[...]
    small = (jnp.zeros((1, width), F32), jnp.zeros((1, width), F32))

    def unit_at(at):
        return (base_ref[at, :].astype(BF16).astype(F32) - mean_ref[at, :]) * rstd_ref[at, :]

    for m in range(MICRO):
        for d in OTHERS:
            copy(m, d).wait()
        sums = []
        for i in range(TOK_DEV // step):
            here = slice(i * step, (i + 1) * step)
            at = slice(m * TOK_DEV + i * step, m * TOK_DEV + (i + 1) * step)
            grad = total_ref[at, :]
            for d in OTHERS:
                grad = grad + recv_buf[m, d - 1, here, :].astype(F32)
            total_ref[at, :] = grad
            unit = unit_at(at)
            product = grad * unit
            small = (
                small[0] + jnp.sum(product, axis=0, keepdims=True),
                small[1] + jnp.sum(grad, axis=0, keepdims=True),
            )
            first = jnp.sum(grad * gain, axis=-1, keepdims=True)
            second = jnp.sum(product * gain, axis=-1, keepdims=True)
            lane = lax.broadcasted_iota(jnp.int32, (step, LANES), 1)
            sums.append(jnp.where(lane == 0, first, jnp.where(lane == 1, second, 0.0)))
        stat_send[m] = jnp.concatenate(sums, axis=0).T[0:8]
        for d in OTHERS:
            stat_copy(m, d).start()
    small_ref[0:1, :] = small[0]
    small_ref[1:2, :] = small[1]

    if spread_it:

        def spread(m, d):
            return remote(
                full_ref.at[r, rows_of(m)],
                full_ref.at[r, rows_of(m)],
                gsend.at[m, d - 1],
                grecv.at[m, d - 1],
                peer_of(r, d),
            )

    for m in range(MICRO):
        sums = stat_send[m]
        for d in OTHERS:
            stat_copy(m, d).wait()
            sums = sums + stat_recv[m, d - 1]
        sums = jnp.concatenate([sums, jnp.zeros((LANES - 8, TOK_DEV), F32)], axis=0).T
        for i in range(TOK_DEV // step):
            at = slice(m * TOK_DEV + i * step, m * TOK_DEV + (i + 1) * step)
            own = sums[i * step : (i + 1) * step]
            value = resid_ref[at, :].astype(F32) + rstd_ref[at, :] * (
                total_ref[at, :] * gain
                - own[:, 0:1] / features
                - unit_at(at) * (own[:, 1:2] / features)
            )
            out_ref[at, :] = value.astype(out_ref.dtype)
            if spread_it:
                full_ref[pl.ds(r, 1), at, :] = value.astype(BF16)[None]
        if spread_it:
            for d in OTHERS:
                spread(m, d).start()
    if spread_it:
        for m in range(MICRO):
            for d in OTHERS:
                spread(m, d).wait()


def back(grads, base, mean, rstd, gain, resid, pieces, spread_it):
    total, width = base.shape
    n = len(grads)
    small = jax.ShapeDtypeStruct((2, width), F32)
    if spread_it:
        out_shape = (
            jax.ShapeDtypeStruct((total, width), F32),
            jax.ShapeDtypeStruct((ROWS, total, width), BF16),
            small,
        )
    else:
        out_shape = (jax.ShapeDtypeStruct((total, width), BF16), small)
    return pl.pallas_call(
        functools.partial(back_kernel, n, spread_it),
        out_shape=out_shape,
        in_specs=[VMEM] * (n + 5) + [HBM] * len(pieces),
        out_specs=(VMEM,) * len(out_shape),
        scratch_shapes=[
            pltpu.VMEM((ROWS, n, width, grads[0].shape[1]), BF16),
            pltpu.VMEM((total, width), F32),
        ]
        + exchange_scratch(width)
        + [
            pltpu.VMEM((MICRO, 8, TOK_DEV), F32),
            pltpu.VMEM((MICRO, 3, 8, TOK_DEV), F32),
            sems(len(pieces)),
            sems(MICRO, 3),
            sems(MICRO, 3),
            sems(2, MICRO, 3),
        ]
        + ([sems(MICRO, 3), sems(MICRO, 3)] if spread_it else []),
        compiler_params=comm_params(4 if spread_it else 5),
        name="back_spread" if spread_it else "back_last",
    )(*grads, base, mean, rstd, gain, resid, *pieces)


def piece_block(ref, b, pieces):
    per_row = pieces // ROWS
    own = ref.shape[2] // per_row
    offset = pl.multiple_of(lax.rem(b, per_row) * own, own)
    return ref[b // per_row, :, pl.ds(offset, own)]


def rotate(chunk, cosine, near, far):
    return chunk * cosine + pltpu.roll(chunk, LANES - 8, 1) * near + pltpu.roll(chunk, 8, 1) * far


def attention_tiles():
    for i in range(TOK_DEV // LANES):
        yield slice(i * LANES, (i + 1) * LANES), (i + 1) * LANES


def head_masks(rows):
    lane = lax.broadcasted_iota(jnp.int32, (rows, LANES), 1)
    return lane < HEAD_DIM


def probabilities(query, keys, allowed, scaling):
    scores = dot(query, keys, 1, 1) * scaling
    scores = jnp.where(allowed > 0, scores, -1e30)
    totals = jnp.log(jnp.sum(jnp.exp(scores), axis=-1, keepdims=True))
    return jnp.exp(scores - totals)


def attention_kernel(scaling, normed_ref, rope_ref, allowed_ref, bias_ref, *refs):
    pieces, (q_ref, k_ref, v_ref, att_ref) = refs[:-4], refs[-4:]
    pairs = len(pieces) // 2
    blocks = [block_of(k, pairs) for k in range(len(pieces))]
    cosine, near, far = rope_ref[0, 0], rope_ref[0, 1], rope_ref[0, 2]
    for i, out_ref in enumerate((q_ref, k_ref, v_ref)):
        for start, size in tiles(out_ref.shape[1]):
            cols = slice(start, start + size)
            mixed = sum(
                dot(piece_block(normed_ref, b, len(pieces)), piece[i, :, cols], 1, 0)
                for b, piece in zip(blocks, pieces)
            )
            mixed = mixed + bias_ref[i : i + 1, cols]
            if i == 2:
                out_ref[:, cols] = mixed.astype(BF16)
                continue
            for part in range(0, size, LANES):
                chunk = rotate(mixed[:, part : part + LANES], cosine, near, far)
                out_ref[:, start + part : start + part + LANES] = chunk.astype(BF16)

    @pl.loop(0, q_ref.shape[1] // LANES)
    def _(h):
        cols = pl.ds(pl.multiple_of(h * LANES, LANES), LANES)
        for rows, count in attention_tiles():
            low = head_masks(LANES)
            query = q_ref[rows, cols]
            keys = k_ref[0:count, cols]
            values = v_ref[0:count, cols]
            allowed = allowed_ref[0, rows, 0:count]
            outs = []
            for mask in (low, ~low):
                probs = probabilities(
                    jnp.where(mask, query, jnp.zeros_like(query)), keys, allowed, scaling
                )
                outs.append(dot(probs.astype(BF16), values, 1, 0))
            att_ref[rows, cols] = jnp.where(low, outs[0], outs[1]).astype(BF16)


def constant(shape):
    return pl.BlockSpec(shape, lambda m: (0,) * len(shape), pipeline_mode=pl.Buffered(1))


def by_micro(shape, axis):
    return pl.BlockSpec(shape, lambda m: tuple(m if i == axis else 0 for i in range(len(shape))))


def estimate(flops, *arrays):
    total = sum(math.prod(a.shape) * a.dtype.itemsize for a in arrays)
    return pl.CostEstimate(flops=flops, bytes_accessed=total, transcendentals=0)


def attention(normed, rope, allowed, bias, pieces):
    width = bias.shape[1]
    total = normed.shape[1]
    out = jax.ShapeDtypeStruct((total, width), BF16)
    return pl.pallas_call(
        functools.partial(attention_kernel, 1.0 / math.sqrt(HEAD_DIM)),
        grid=(MICRO,),
        out_shape=(out,) * 4,
        in_specs=[
            by_micro((ROWS, TOK_DEV, normed.shape[2]), 1),
            by_micro((1,) + rope.shape[1:], 0),
            by_micro((1, TOK_DEV, TOK_DEV), 0),
            constant(bias.shape),
        ]
        + [constant(piece.shape) for piece in pieces],
        out_specs=(by_micro((TOK_DEV, width), 0),) * 4,
        cost_estimate=estimate(8 * total * ROWS * normed.shape[2] * width, normed, *pieces),
        name="attention",
    )(normed, rope, allowed, bias, *pieces)


def gate_up_kernel(normed_ref, *refs):
    pieces, (gate_ref, up_ref, act_ref) = refs[:-3], refs[-3:]
    pairs = len(pieces) // 2
    blocks = [block_of(k, pairs) for k in range(len(pieces))]
    for start, size in tiles(gate_ref.shape[1]):
        cols = slice(start, start + size)
        gate, up = [
            sum(
                dot(piece_block(normed_ref, b, len(pieces)), piece[i, :, cols], 1, 0)
                for b, piece in zip(blocks, pieces)
            )
            for i in range(2)
        ]
        gate_ref[:, cols] = gate
        up_ref[:, cols] = up
        act_ref[:, cols] = (gate / (1.0 + jnp.exp(-gate)) * up).astype(BF16)


def gate_up(normed, pieces):
    total, width = normed.shape[1], pieces[0].shape[2]
    return pl.pallas_call(
        gate_up_kernel,
        grid=(MICRO,),
        out_shape=(
            jax.ShapeDtypeStruct((total, width), F32),
            jax.ShapeDtypeStruct((total, width), F32),
            jax.ShapeDtypeStruct((total, width), BF16),
        ),
        in_specs=[by_micro((ROWS, TOK_DEV, normed.shape[2]), 1)]
        + [constant(piece.shape) for piece in pieces],
        out_specs=(by_micro((TOK_DEV, width), 0),) * 3,
        cost_estimate=estimate(4 * total * ROWS * normed.shape[2] * width, normed, *pieces),
        name="gate_up",
    )(normed, *pieces)


def mlp_back_kernel(grad_ref, gate_ref, up_ref, *refs):
    pieces, (dgate_ref, dup_ref) = refs[:-2], refs[-2:]
    pairs = len(pieces) // 2
    blocks = [block_of(k, pairs) for k in range(len(pieces))]
    for start, size in tiles(gate_ref.shape[1]):
        cols = slice(start, start + size)
        grad = sum(
            dot(piece_block(grad_ref, b, len(pieces)), piece[cols, :], 1, 1)
            for b, piece in zip(blocks, pieces)
        )
        gate, up = gate_ref[:, cols], up_ref[:, cols]
        sigmoid = 1.0 / (1.0 + jnp.exp(-gate))
        dgate_ref[:, cols] = (grad * up * sigmoid * (1.0 + gate * (1.0 - sigmoid))).astype(BF16)
        dup_ref[:, cols] = (grad * (gate * sigmoid)).astype(BF16)


def mlp_back(grad_full, gate, up, pieces):
    total, width = gate.shape
    out = jax.ShapeDtypeStruct((total, width), BF16)
    return pl.pallas_call(
        mlp_back_kernel,
        grid=(MICRO,),
        out_shape=(out, out),
        in_specs=[
            by_micro((ROWS, TOK_DEV, grad_full.shape[2]), 1),
            by_micro((TOK_DEV, width), 0),
            by_micro((TOK_DEV, width), 0),
        ]
        + [constant(piece.shape) for piece in pieces],
        out_specs=(by_micro((TOK_DEV, width), 0),) * 2,
        cost_estimate=estimate(2 * total * ROWS * grad_full.shape[2] * width, gate, up, *pieces),
        name="mlp_back",
    )(grad_full, gate, up, *pieces)


def attention_back_kernel(
    scaling, grad_ref, q_ref, k_ref, v_ref, rope_ref, allowed_ref, *refs
):
    pieces, refs = refs[:-6], refs[-6:]
    (dq_ref, dk_ref, dv_ref, bias_ref, dk_sum, dv_sum) = refs
    pairs = len(pieces) // 2
    blocks = [block_of(k, pairs) for k in range(len(pieces))]
    for start, size in tiles(dq_ref.shape[1]):
        cols = slice(start, start + size)
        grad = sum(
            dot(piece_block(grad_ref, b, len(pieces)), piece[cols, :], 1, 1)
            for b, piece in zip(blocks, pieces)
        )
        dq_ref[:, cols] = grad.astype(BF16)
    cosine, near, far = rope_ref[0, 0], rope_ref[0, 1], rope_ref[0, 2]

    @pl.loop(0, q_ref.shape[1] // LANES)
    def _(h):
        cols = pl.ds(pl.multiple_of(h * LANES, LANES), LANES)
        dk_sum[...] = jnp.zeros_like(dk_sum)
        dv_sum[...] = jnp.zeros_like(dv_sum)
        bias = [jnp.zeros((1, LANES), F32) for _ in range(3)]
        for rows, count in attention_tiles():
            low = head_masks(LANES)
            query, grad = q_ref[rows, cols], dq_ref[rows, cols]
            keys, values = k_ref[0:count, cols], v_ref[0:count, cols]
            allowed = allowed_ref[0, rows, 0:count]
            dqs, dks, dvs = [], [], []
            for mask in (low, ~low):
                own_query = jnp.where(mask, query, jnp.zeros_like(query))
                own_grad = jnp.where(mask, grad, jnp.zeros_like(grad))
                probs = probabilities(own_query, keys, allowed, scaling)
                dprobs = dot(own_grad, values, 1, 1)
                inner = jnp.sum(probs * dprobs, axis=-1, keepdims=True)
                dscores = (probs * (dprobs - inner)).astype(BF16)
                dqs.append(dot(dscores, keys, 1, 0))
                dks.append(dot(dscores, own_query, 0, 0))
                dvs.append(dot(probs.astype(BF16), own_grad, 0, 0))
            dk_sum[0:count, :] += dks[0] + dks[1]
            dv_sum[0:count, :] += dvs[0] + dvs[1]
            dq = jnp.where(low, dqs[0], dqs[1]) * scaling
            dq = rotate(dq, cosine[rows], -near[rows], -far[rows]).astype(BF16)
            dq_ref[rows, cols] = dq
            bias[0] = bias[0] + jnp.sum(dq.astype(F32), axis=0, keepdims=True)
        dk = rotate(dk_sum[...] * scaling, cosine, -near, -far).astype(BF16)
        dk_ref[:, cols] = dk
        dv = dv_sum[...].astype(BF16)
        dv_ref[:, cols] = dv
        bias[1] = jnp.sum(dk.astype(F32), axis=0, keepdims=True)
        bias[2] = jnp.sum(dv.astype(F32), axis=0, keepdims=True)
        for i in range(3):
            bias_ref[0, i : i + 1, cols] = bias[i]


def attention_back(grad_full, queries, keys, values, rope, allowed, pieces):
    total, width = queries.shape
    out = jax.ShapeDtypeStruct((total, width), BF16)
    block = by_micro((TOK_DEV, width), 0)
    return pl.pallas_call(
        functools.partial(attention_back_kernel, 1.0 / math.sqrt(HEAD_DIM)),
        grid=(MICRO,),
        out_shape=(out, out, out, jax.ShapeDtypeStruct((MICRO, 3, width), F32)),
        in_specs=[
            by_micro((ROWS, TOK_DEV, grad_full.shape[2]), 1),
            block,
            block,
            block,
            by_micro((1,) + rope.shape[1:], 0),
            by_micro((1, TOK_DEV, TOK_DEV), 0),
        ]
        + [constant(piece.shape) for piece in pieces],
        out_specs=(block, block, block, by_micro((1, 3, width), 0)),
        scratch_shapes=[pltpu.VMEM((TOK_DEV, LANES), F32)] * 2,
        cost_estimate=estimate(4 * total * ROWS * grad_full.shape[2] * width, queries, *pieces),
        name="attention_back",
    )(grad_full, queries, keys, values, rope, allowed, *pieces)


def weight_grad_kernel(n, cols, left_blocked, *refs):
    left_ref, rights, (keep_ref, give_ref) = refs[0], refs[1 : 1 + n], refs[1 + n :]
    k = pl.program_id(0)
    pairs = cols // 2
    b = lax.rem(lax.axis_index("section") + k // pairs, 2) * pairs + lax.rem(
        lax.axis_index("pair") + lax.rem(k, pairs), pairs
    )
    for out_ref, mine in ((keep_ref, k < pairs), (give_ref, k >= pairs)):

        @pl.when(mine)
        def _(out_ref=out_ref):
            if left_blocked:
                left = piece_block(left_ref, b, cols)
                for i in range(n):
                    for start, size in tiles(rights[i].shape[1], 2 * WIDE):
                        at = slice(start, start + size)
                        out_ref[0, i, :, at] = dot(left, rights[i][:, at], 0, 0).astype(BF16)
            else:
                right = piece_block(rights[0], b, cols)
                for start, size in tiles(left_ref.shape[1], 2 * WIDE):
                    at = slice(start, start + size)
                    out_ref[0, 0, at, :] = dot(left_ref[:, at], right, 0, 0).astype(BF16)


def weight_grad(left, rights, cols, left_blocked, name):
    n = len(rights)
    blocked = left if left_blocked else rights[0]
    own = ROWS * blocked.shape[2] // cols
    if left_blocked:
        shard = (n, own, rights[0].shape[1])
    else:
        shard = (1, left.shape[1], own)
    pairs = cols // 2
    out = jax.ShapeDtypeStruct((pairs,) + shard, BF16)
    return pl.pallas_call(
        functools.partial(weight_grad_kernel, n, cols, left_blocked),
        grid=(cols,),
        out_shape=(out, out),
        in_specs=[constant(a.shape) for a in (left, *rights)],
        out_specs=(
            pl.BlockSpec((1,) + shard, lambda k: (jnp.minimum(k, pairs - 1), 0, 0, 0)),
            pl.BlockSpec((1,) + shard, lambda k: (jnp.maximum(k - pairs, 0), 0, 0, 0)),
        ),
        cost_estimate=estimate(
            2 * cols * math.prod(shard) * blocked.shape[1], left, *rights, out, out
        ),
        name=name,
    )(left, *rights)


class Moves:
    def __init__(self):
        self.pairs = lax.axis_size("pair")
        self.cols = 2 * self.pairs
        self.s = lax.axis_index("section")
        self.g = lax.axis_index("half")

    def send(self, value, moves):
        def flat(r, place):
            s, h, p = place
            return ((s * ROWS + r) * 2 + h) * self.pairs + p

        pairs = [(flat(r, a), flat(r, b)) for r in range(ROWS) for a, b in moves]
        return lax.ppermute(value, AXES, pairs)

    def places(self):
        return [(s, h, p) for s in range(2) for h in range(2) for p in range(self.pairs)]

    def swap(self, value):
        return self.send(
            value, [((s, h, p), (s, h, p) if s == h else (h, s, p)) for s, h, p in self.places()]
        )

    def across(self, value):
        return self.send(value, [((s, h, p), (1 - s, h, p)) for s, h, p in self.places()])

    def along(self, value, j):
        return self.send(
            value, [((s, h, (p + j) % self.pairs), (s, h, p)) for s, h, p in self.places()]
        )

    def back_along(self, value, j):
        return self.send(
            value, [((s, h, p), (s, h, (p + j) % self.pairs)) for s, h, p in self.places()]
        )

    def homes(self):
        for g in range(2):
            for b in range(self.cols):
                yield (g, b // self.pairs, b % self.pairs), (b % 2, g, b // 2)

    def fetch_blocks(self, value):
        return self.send(value, list(self.homes()))

    def return_blocks(self, value):
        return self.send(value, [(b, a) for a, b in self.homes()])

    def hand_on(self, value, forward):
        moves = []
        for s in range(2):
            for p in range(self.pairs):
                a, b = (s, 0, p), (s, 1, p)
                moves.append((a, b) if forward else (b, a))
        return self.send(value, moves)

    def gather_shards(self, own):
        near = [self.swap(own)]
        near += [self.along(near[0], j) for j in range(1, self.pairs)]
        return near + [self.across(shard) for shard in near]

    def scatter_grads(self, keep, give):
        got = self.across(give)
        sums = [keep[j].astype(F32) + got[j].astype(F32) for j in range(self.pairs)]
        total = sums[0]
        for j in range(1, self.pairs):
            total = total + self.back_along(sums[j].astype(BF16), j).astype(F32)
        return self.swap(total.astype(BF16)).astype(F32)

    def total_small(self, value):
        value = value + self.across(value)
        total = value
        for j in range(1, self.pairs):
            total = total + self.along(value, j)
        return self.swap(total)


def layout(seq_lengths):
    end_points = jnp.cumsum(seq_lengths)
    places = jnp.arange(TOK_DEV, dtype=jnp.int32)
    passed = places[:, None] >= end_points[None, :]
    segment = jnp.sum(passed.astype(jnp.int32), axis=1)
    starts = jnp.sum(jnp.where(passed, seq_lengths[None, :], 0), axis=1)
    offset = (places - starts).astype(F32)
    allowed = (segment[:, None] == segment[None, :]) & (places[None, :] <= places[:, None])
    frequency = 10000.0 ** (-(jnp.arange(ROT // 2, dtype=F32) * 2.0 / ROT))
    angles = offset[:, None] * frequency[None, :]
    cosine, sine = jnp.cos(angles), jnp.sin(angles)
    rest = HEAD_DIM - ROT
    nothing = jnp.zeros_like(sine)
    tail = jnp.zeros((TOK_DEV, rest), F32)

    def lanes(*parts):
        head = jnp.concatenate(parts, axis=1)
        return jnp.concatenate([head, head], axis=1)

    rope = jnp.stack(
        [
            lanes(cosine, cosine, tail + 1.0),
            lanes(-sine, nothing, tail),
            lanes(nothing, sine, tail),
        ]
    )
    return allowed.astype(F32), rope


def on_device(
    inputs, lengths, norm_gain, norm_bias, w_qkv, b_qkv, w_out, w_gate_up, w_down, grad_out
):
    moves = Moves()
    width = inputs.shape[2]
    is_first = moves.g == 0

    start = moves.fetch_blocks(jnp.where(moves.s == 0, inputs, grad_out))
    start = start.reshape(MICRO * TOK_DEV, width)
    par = jnp.concatenate([norm_gain[0], norm_bias[0], b_qkv[0], jnp.zeros((1, width), F32)])
    par = moves.swap(par)
    own_lengths = moves.fetch_blocks(lengths)[:, 0]
    tables = [layout(own_lengths[m]) for m in range(MICRO)]
    allowed = jnp.stack([table[0] for table in tables])
    rope = jnp.stack([table[1] for table in tables])

    shards_qkv = moves.gather_shards(jnp.swapaxes(w_qkv[0], 0, 1))
    shards_out = moves.gather_shards(w_out[0])
    shards_gate_up = moves.gather_shards(jnp.swapaxes(w_gate_up[0], 0, 1))
    shards_down = moves.gather_shards(w_down[0])

    def forward(x):
        full_one, normed_one, par_full, mean_one, rstd_one = gather_norm(x, par)
        queries, keys, values, attended = attention(
            normed_one, rope, allowed, par[4:7], shards_qkv
        )
        hidden, _, normed_two, mean_two, rstd_two = out_norm(attended, x, par_full, shards_out)
        gate, up, activated = gate_up(normed_two, shards_gate_up)
        out = down(activated, hidden, shards_down)
        return out, full_one, (
            (x, normed_one, mean_one, rstd_one),
            (queries, keys, values, attended),
            (hidden, normed_two, mean_two, rstd_two),
            (gate, up, activated),
        )

    def backward(grad, grad_full, saved):
        one, heads, two, mlp = saved
        x, normed_one, mean_one, rstd_one = one
        queries, keys, values, attended = heads
        hidden, normed_two, mean_two, rstd_two = two
        gate, up, activated = mlp
        cols = moves.cols
        dgate, dup = mlp_back(grad_full, gate, up, shards_down)
        for_down = weight_grad(activated, [grad_full], cols, False, "grad_down")
        for_gate_up = weight_grad(normed_two, [dgate, dup], cols, True, "grad_gate_up")
        dhidden, dhidden_full, small_two = back(
            [dgate, dup], hidden, mean_two, rstd_two, par[1:2], grad, shards_gate_up, True
        )
        dq, dk, dv, dbias = attention_back(
            dhidden_full, queries, keys, values, rope, allowed, shards_out
        )
        for_out = weight_grad(attended, [dhidden_full], cols, False, "grad_out")
        for_qkv = weight_grad(normed_one, [dq, dk, dv], cols, True, "grad_qkv")
        dx, small_one = back(
            [dq, dk, dv], x, mean_one, rstd_one, par[0:1], dhidden, shards_qkv, False
        )
        small = jnp.concatenate(
            [
                small_one[0:1],
                small_two[0:1],
                small_one[1:2],
                small_two[1:2],
                jnp.sum(dbias, axis=0),
                jnp.zeros((1, width), F32),
            ]
        )
        return dx, small, (for_qkv, for_out, for_gate_up, for_down)

    out_first, start_full, saved_first = forward(start)
    out_second, _, saved_second = forward(moves.hand_on(out_first, True))
    activations = moves.return_blocks(jnp.where(is_first, out_first, out_second))
    grad_second, small_second, large_second = backward(start, start_full, saved_second)
    handed = moves.hand_on(grad_second, False)
    grad_first, small_first, large_first = backward(handed, gather(handed), saved_first)
    input_grad = moves.return_blocks(jnp.where(is_first, grad_first, grad_second))

    parts = [
        moves.scatter_grads(*[jnp.where(is_first, a, b) for a, b in zip(first, second)])
        for first, second in zip(large_first, large_second)
    ]
    sums = moves.total_small(jnp.where(is_first, small_first, small_second))
    return (
        activations.reshape(1, MICRO, TOK_DEV, width),
        input_grad.reshape(1, MICRO, TOK_DEV, width),
        sums[None, 0:2],
        sums[None, 2:4],
        jnp.swapaxes(parts[0], 0, 1)[None],
        sums[None, 4:7],
        parts[1],
        jnp.swapaxes(parts[2], 0, 1)[None],
        parts[3],
    )


def solution(mesh):
    cols = mesh.shape["col"]
    halves = Mesh(
        mesh.devices.reshape(2, mesh.shape["row"], 2, cols // 2), AXES
    )
    col = ("half", "pair")
    in_specs = (
        P(None, col, "row"),
        P(None, col, None),
        P("section", None, "row"),
        P("section", None, "row"),
        P("section", col, None, "row"),
        P("section", None, "row"),
        P("section", "row", col),
        P("section", col, None, "row"),
        P("section", "row", col),
        P(None, col, "row"),
    )
    out_specs = (
        P("section", None, col, "row"),
        P("section", None, col, "row"),
        P("section", None, "row"),
        P("section", None, "row"),
        P("section", col, None, "row"),
        P("section", None, "row"),
        P("section", "row", col),
        P("section", col, None, "row"),
        P("section", "row", col),
    )
    return jax.shard_map(
        on_device, mesh=halves, in_specs=in_specs, out_specs=out_specs, check_vma=False
    )
```

```python
import functools
import math

import jax
import jax.numpy as jnp
from jax import lax
from jax.experimental import pallas as pl
from jax.experimental.pallas import tpu as pltpu
from jax.sharding import Mesh
from jax.sharding import PartitionSpec as P


HEAD_DIM = 64
ROT = 16
TOK_DEV = 384
MICRO = 2
EPSILON = 1e-05
LANES = 128
WIDE = 256
AXES = SEC, ROW, GROUP, PAIR = ("section", "row", "half", "pair")
COL = (GROUP, PAIR)
BF16 = jnp.bfloat16
F32 = jnp.float32
MESH = pl.DeviceIdType.MESH
VMEM = pl.BlockSpec(memory_space=pltpu.VMEM)
HBM = pl.BlockSpec(memory_space=pl.ANY)


def dot(left, right, left_dim, right_dim):
    return lax.dot_general(
        left, right, (((left_dim,), (right_dim,)), ((), ())), preferred_element_type=F32
    )


def block_of(k, pairs):
    half = lax.rem(lax.axis_index(SEC) + k // pairs, 2)
    return half * pairs + lax.rem(lax.axis_index(PAIR) + k % pairs, pairs)


def tiles(width, tile=WIDE):
    return [(start, min(tile, width - start)) for start in range(0, width, tile)]


def peer_of(r, d):
    return lax.rem(r // 2 + d // 2, 2) * 2 + lax.rem(lax.rem(r, 2) + d % 2, 2)


SPREAD, HAND, LAST = range(3)
ROWS = 4
NEAR = (1, 2)
HALF = TOK_DEV // 2


def greet(targets, count):
    barrier = pltpu.get_barrier_semaphore()
    for target in targets:
        pl.semaphore_signal(barrier, inc=1, device_id=target, device_id_type=MESH)
    pl.semaphore_wait(barrier, count)


def row_barrier(r, hand=False):
    targets = [{ROW: peer_of(r, d)} for d in NEAR]
    if hand:
        targets.append({GROUP: 1 - lax.axis_index(GROUP)})
    greet(targets, len(targets))


def remote(source, target, send_sem, recv_sem, device):
    return pltpu.make_async_remote_copy(
        src_ref=source,
        dst_ref=target,
        send_sem=send_sem,
        recv_sem=recv_sem,
        device_id=device,
        device_id_type=MESH,
    )


def rows_of(m):
    return pl.ds(m * TOK_DEV, TOK_DEV)


def half_of(m, d):
    return pl.ds(m * TOK_DEV + (d - 1) * HALF, HALF)


class Spread:
    def __init__(self, r, full_ref, semaphores):
        self.r, self.full_ref, self.sems = r, full_ref, semaphores

    def direct(self, m, d):
        block = self.full_ref.at[self.r, rows_of(m)]
        return remote(
            block,
            block,
            self.sems.at[0, m, d - 1],
            self.sems.at[1, m, d - 1],
            {ROW: peer_of(self.r, d)},
        )

    def onward(self, m, d):
        block = self.full_ref.at[peer_of(self.r, 3 - d), half_of(m, 3 - d)]
        return remote(
            block,
            block,
            self.sems.at[2, m, d - 1],
            self.sems.at[3, m, d - 1],
            {ROW: peer_of(self.r, d)},
        )

    def start(self, m):
        for d in NEAR:
            self.direct(m, d).start()

    def relay(self, m):
        for d in NEAR:
            self.direct(m, d).wait_recv()
            self.onward(m, 3 - d).start()

    def finish(self, m):
        for d in NEAR:
            self.onward(m, d).wait_recv()

    def drain(self):
        for m in range(MICRO):
            for d in NEAR:
                self.direct(m, d).wait_send()
                self.onward(m, d).wait_send()


def sems(*shape):
    return pltpu.SemaphoreType.DMA(shape)


SPREAD_SEMS = (4, MICRO, 2)


def comm_params(collective_id):
    return pltpu.CompilerParams(collective_id=collective_id, has_side_effects=True)


def wire_estimate(flops=0):
    return pl.CostEstimate(flops=flops + 30_000_000_000, bytes_accessed=0, transcendentals=0)


def layer_norm(full_ref, out_ref, mean_ref, rstd_ref, gain_of, shift_of, first, rows):
    step = 32
    count = full_ref.shape[0] * full_ref.shape[2]

    @pl.loop(0, rows // step)
    def _(i):
        at = pl.ds(pl.multiple_of(first + i * step, step), step)
        total = jnp.zeros((step, 1), F32)
        square = jnp.zeros((step, 1), F32)
        for b in range(full_ref.shape[0]):
            block = full_ref[b, at, :].astype(F32)
            total = total + jnp.sum(block, axis=-1, keepdims=True)
            square = square + jnp.sum(block * block, axis=-1, keepdims=True)
        mean = total / count
        rstd = lax.rsqrt(square / count - mean * mean + EPSILON)
        mean_ref[at, :] = mean
        rstd_ref[at, :] = rstd
        for b in range(full_ref.shape[0]):
            unit = (full_ref[b, at, :].astype(F32) - mean) * rstd
            out_ref[b, at, :] = (unit * gain_of(b) + shift_of(b)).astype(BF16)


def gather_kernel(
    x_ref, par_ref, full_ref, par_full_ref, par_out_ref, mate_ref, spread_sems, par_sems, mate_sems
):
    r, s = lax.axis_index(ROW), lax.axis_index(SEC)
    greet([{ROW: peer_of(r, d)} for d in (1, 2, 3)] + [{SEC: 1 - s}], 4)
    spread = Spread(r, full_ref, spread_sems)
    mate = remote(par_ref, mate_ref, mate_sems.at[0], mate_sems.at[1], {SEC: 1 - s})
    mate.start()
    full_ref[pl.ds(r, 1)] = x_ref[...][None]
    for m in range(MICRO):
        spread.start(m)
    mate.wait()
    own = (s == lax.axis_index(GROUP)).astype(F32)
    par = par_ref[...] * own + mate_ref[...] * (1.0 - own)
    par_out_ref[...] = par
    par_full_ref[pl.ds(r, 1)] = par[None]

    def par_copy(d):
        return remote(
            par_out_ref,
            par_full_ref.at[r],
            par_sems.at[0, d - 1],
            par_sems.at[1, d - 1],
            {ROW: peer_of(r, d)},
        )

    for d in (3, 1, 2):
        par_copy(d).start()
    for m in range(MICRO):
        spread.relay(m)
    for m in range(MICRO):
        spread.finish(m)
    for d in (3, 1, 2):
        par_copy(d).wait()
    spread.drain()


def gather(x, par):
    return pl.pallas_call(
        gather_kernel,
        out_shape=(
            jax.ShapeDtypeStruct((ROWS,) + x.shape, BF16),
            jax.ShapeDtypeStruct((ROWS,) + par.shape, F32),
            jax.ShapeDtypeStruct(par.shape, F32),
        ),
        in_specs=[VMEM, VMEM],
        out_specs=(VMEM,) * 3,
        scratch_shapes=[pltpu.VMEM(par.shape, F32), sems(*SPREAD_SEMS), sems(2, 3), sems(2)],
        compiler_params=comm_params(0),
        cost_estimate=wire_estimate(),
    )(x, par)


def load_blocks(piece_refs, buffer, sem, width, by_columns):
    pairs = len(piece_refs) // 2
    own = width // len(piece_refs)
    per_row = len(piece_refs) // ROWS
    copies = []
    for k, piece in enumerate(piece_refs):
        b = block_of(k, pairs)
        at = pl.ds(pl.multiple_of(lax.rem(b, per_row) * own, own), own)
        target = buffer.at[b // per_row, :, at]
        if not by_columns:
            target = buffer.at[b // per_row, :, at, :]
        copies.append(pltpu.make_async_copy(piece, target, sem.at[k]))
    for copy in copies:
        copy.start()
    return copies


class Exchange:
    def __init__(self, r, scratch):
        self.r = r
        self.send_buf, self.relay_buf, self.recv_buf, self.sems = scratch

    def direct(self, m, d):
        return remote(
            self.send_buf.at[m, d - 1],
            self.recv_buf.at[m, d - 1],
            self.sems.at[0, m, d - 1],
            self.sems.at[1, m, d - 1],
            {ROW: peer_of(self.r, d)},
        )

    def relay(self, m, d):
        return remote(
            self.send_buf.at[m, 2, pl.ds((d - 1) * HALF, HALF)],
            self.relay_buf.at[m, d - 1],
            self.sems.at[2, m, d - 1],
            self.sems.at[3, m, d - 1],
            {ROW: peer_of(self.r, d)},
        )

    def start(self, partial, own_ref):
        width = own_ref.shape[1]
        columns = [slice(start, start + size) for start, size in tiles(width)]
        for m in range(MICRO):
            for cols in columns:
                part = partial(m, peer_of(self.r, 3), cols)
                self.send_buf[m, 2, :, cols] = part.astype(BF16)
            for d in NEAR:
                self.relay(m, d).start()
        for m in range(MICRO):
            for cols in columns:
                own_ref[rows_of(m), cols] = partial(m, self.r, cols)
        for m in range(MICRO):
            for d in NEAR:
                self.relay(m, 3 - d).wait_recv()
                added = slice(HALF, TOK_DEV) if d == 1 else slice(0, HALF)
                kept = slice(0, HALF) if d == 1 else slice(HALF, TOK_DEV)
                for cols in columns:
                    part = partial(m, peer_of(self.r, d), cols)
                    passed = self.relay_buf[m, 2 - d, :, cols].astype(F32)
                    self.send_buf[m, d - 1, kept, cols] = part[kept].astype(BF16)
                    self.send_buf[m, d - 1, added, cols] = (part[added] + passed).astype(BF16)
                self.direct(m, d).start()

    def wait(self, m):
        for d in NEAR:
            self.direct(m, d).wait_recv()

    def received(self, m, rows):
        return self.recv_buf[m, 0, rows, :].astype(F32) + self.recv_buf[m, 1, rows, :].astype(F32)

    def drain(self):
        for m in range(MICRO):
            for d in NEAR:
                self.direct(m, d).wait_send()
                self.relay(m, d).wait_send()


def exchange_scratch(width):
    return [
        pltpu.VMEM((MICRO, 3, TOK_DEV, width), BF16),
        pltpu.VMEM((MICRO, 2, HALF, width), BF16),
        pltpu.VMEM((MICRO, 2, TOK_DEV, width), BF16),
        sems(4, MICRO, 2),
    ]


def row_steps(m, step=64):
    for i in range(TOK_DEV // step):
        first = m * TOK_DEV + i * step
        yield slice(i * step, (i + 1) * step), slice(first, first + step)


def out_norm_kernel(*refs):
    (att_ref, x_ref, par_full_ref), refs = refs[:3], refs[3:]
    pieces, refs = refs[:-12], refs[-12:]
    (hidden_ref, full_ref, normed_ref, mean_ref, rstd_ref, weight, wsem), refs = refs[:7], refs[7:]
    r = lax.axis_index(ROW)
    loads = load_blocks(pieces, weight, wsem, ROWS * hidden_ref.shape[1], True)
    row_barrier(r)
    for load in loads:
        load.wait()

    def partial(m, owner, cols):
        return dot(att_ref[rows_of(m), :], weight[owner, :, cols], 1, 0)

    exchange = Exchange(r, refs[:4])
    spread = Spread(r, full_ref, refs[4])
    exchange.start(partial, hidden_ref)
    for m in range(MICRO):
        exchange.wait(m)
        for here, at in row_steps(m):
            hidden = hidden_ref[at, :] + x_ref[at, :].astype(F32) + exchange.received(m, here)
            hidden_ref[at, :] = hidden
            full_ref[pl.ds(r, 1), at, :] = hidden.astype(BF16)[None]
        spread.start(m)
    for m in range(MICRO):
        spread.relay(m)
    for m in range(MICRO):
        spread.finish(m)
        layer_norm(
            full_ref,
            normed_ref,
            mean_ref,
            rstd_ref,
            lambda b: par_full_ref[b, 1:2, :],
            lambda b: par_full_ref[b, 3:4, :],
            m * TOK_DEV,
            TOK_DEV,
        )
    exchange.drain()
    spread.drain()


def out_norm(attended, x, par_full, pieces):
    total, width = x.shape
    return pl.pallas_call(
        out_norm_kernel,
        out_shape=(
            jax.ShapeDtypeStruct((total, width), F32),
            jax.ShapeDtypeStruct((ROWS, total, width), BF16),
            jax.ShapeDtypeStruct((ROWS, total, width), BF16),
            jax.ShapeDtypeStruct((total, 1), F32),
            jax.ShapeDtypeStruct((total, 1), F32),
        ),
        in_specs=[VMEM] * 3 + [HBM] * len(pieces),
        out_specs=(VMEM,) * 5,
        scratch_shapes=[pltpu.VMEM((ROWS, attended.shape[1], width), BF16), sems(len(pieces))]
        + exchange_scratch(width)
        + [sems(*SPREAD_SEMS)],
        compiler_params=comm_params(2),
        cost_estimate=wire_estimate(30_000_000_000),
    )(attended, x, par_full, *pieces)


class Hand:
    def __init__(self, r, source, out_ref, next_ref, full_ref, hand_sems, spread_sems):
        self.r, self.source = r, source
        self.out_ref, self.next_ref, self.full_ref = out_ref, next_ref, full_ref
        self.sems = hand_sems
        self.spread = Spread(r, full_ref, spread_sems)
        self.half = lax.axis_index(GROUP)

    def copy(self, m):
        return remote(
            self.out_ref.at[rows_of(m)],
            self.full_ref.at[self.r, rows_of(m)],
            self.sems.at[0, m],
            self.sems.at[1, m],
            {GROUP: 1 - self.half},
        )

    def start(self, m):
        @pl.when(self.half == self.source)
        def _():
            self.copy(m).start()
            self.full_ref[pl.ds(self.r, 1), rows_of(m), :] = self.out_ref[rows_of(m), :][None]

    def finish(self):
        for m in range(MICRO):

            @pl.when(self.half != self.source)
            def _():
                self.copy(m).wait_recv()

            self.spread.start(m)
            if m:
                self.spread.relay(m - 1)
            self.next_ref[rows_of(m), :] = self.full_ref[pl.ds(self.r, 1), rows_of(m), :][0]
        self.spread.relay(MICRO - 1)
        for m in range(MICRO):
            self.spread.finish(m)

            @pl.when(self.half == self.source)
            def _():
                self.copy(m).wait_send()

        self.spread.drain()


def hand_shapes(total, width):
    return (
        jax.ShapeDtypeStruct((total, width), BF16),
        jax.ShapeDtypeStruct((ROWS, total, width), BF16),
    )


HAND_SCRATCH = (sems(2, MICRO), sems(*SPREAD_SEMS))


class Down:
    def __init__(self, r, act_ref, hidden_ref, out_ref, weight, total_ref, scratch):
        self.act_ref, self.hidden_ref, self.out_ref = act_ref, hidden_ref, out_ref
        self.weight, self.total_ref = weight, total_ref
        self.exchange = Exchange(r, scratch)

    def partial(self, m, owner, cols):
        return dot(self.act_ref[rows_of(m), :], self.weight[owner, :, cols], 1, 0)

    def start(self):
        self.exchange.start(self.partial, self.total_ref)

    def finish(self, m):
        self.exchange.wait(m)
        for here, at in row_steps(m):
            value = self.hidden_ref[at, :] + self.total_ref[at, :]
            value = value + self.exchange.received(m, here)
            self.out_ref[at, :] = value.astype(BF16)


def down_scratch(rows, width, hidden, count):
    return [
        pltpu.VMEM((ROWS, hidden, width), BF16),
        pltpu.VMEM((rows, width), F32),
        sems(count),
    ] + exchange_scratch(width)


def down_kernel(act_ref, hidden_ref, *refs):
    pieces, refs = refs[:-12], refs[-12:]
    (out_ref, next_ref, full_ref, weight, total_ref, wsem), refs = refs[:6], refs[6:]
    r = lax.axis_index(ROW)
    loads = load_blocks(pieces, weight, wsem, ROWS * hidden_ref.shape[1], True)
    row_barrier(r, True)
    for load in loads:
        load.wait()
    down = Down(r, act_ref, hidden_ref, out_ref, weight, total_ref, refs[:4])
    hand = Hand(r, 0, out_ref, next_ref, full_ref, *refs[4:])
    down.start()
    for m in range(MICRO):
        down.finish(m)
        hand.start(m)
    hand.finish()
    down.exchange.drain()


def down_and_hand(activated, hidden, pieces):
    total, width = hidden.shape
    out = (jax.ShapeDtypeStruct((total, width), BF16),) + hand_shapes(total, width)
    return pl.pallas_call(
        down_kernel,
        out_shape=out,
        in_specs=[VMEM] * 2 + [HBM] * len(pieces),
        out_specs=(VMEM,) * len(out),
        scratch_shapes=down_scratch(total, width, activated.shape[1], len(pieces))
        + list(HAND_SCRATCH),
        compiler_params=comm_params(3),
        cost_estimate=wire_estimate(),
    )(activated, hidden, *pieces)


def down_last_kernel(act_ref, hidden_ref, *refs):
    pieces, refs = refs[:-8], refs[-8:]
    (out_ref, weight, total_ref, wsem), refs = refs[:4], refs[4:]
    r = lax.axis_index(ROW)
    loads = load_blocks(pieces, weight, wsem, ROWS * hidden_ref.shape[1], True)
    row_barrier(r)
    for load in loads:
        load.wait()
    down = Down(r, act_ref, hidden_ref, out_ref, weight, total_ref, refs)
    down.start()
    for m in range(MICRO):
        down.finish(m)
    down.exchange.drain()


def trade_kernel(grad_ref, out_ref):
    for i in range(grad_ref.shape[0]):
        out_ref[:, i, :] = grad_ref[i].astype(F32)


def trade(grad):
    n, rows, width = grad.shape
    count = 4
    part = rows // count
    return pl.pallas_call(
        trade_kernel,
        grid=(count,),
        out_shape=jax.ShapeDtypeStruct((rows, n, width), F32),
        in_specs=[pl.BlockSpec((n, part, width), lambda i: (0, i, 0))],
        out_specs=pl.BlockSpec((part, n, width), lambda i: (i, 0, 0)),
        cost_estimate=pl.CostEstimate(
            flops=0, bytes_accessed=6 * math.prod(grad.shape), transcendentals=0
        ),
    )(grad)


def down_last(activated, hidden, pieces):
    total, width = hidden.shape
    return pl.pallas_call(
        down_last_kernel,
        out_shape=jax.ShapeDtypeStruct((total, width), BF16),
        in_specs=[VMEM] * 2 + [HBM] * len(pieces),
        out_specs=VMEM,
        scratch_shapes=down_scratch(total, width, activated.shape[1], len(pieces)),
        compiler_params=comm_params(6),
        cost_estimate=wire_estimate(),
    )(activated, hidden, *pieces)


def back_kernel(n, mode, *refs):
    grads, refs = refs[:n], refs[n:]
    (base_ref, mean_ref, rstd_ref, gain_ref, resid_ref), refs = refs[:5], refs[5:]
    tail = (14, 16, 12)[mode]
    pieces, refs = refs[:-tail], refs[-tail:]
    out_ref, small_ref, refs = refs[0], refs[1], refs[2:]
    if mode == SPREAD:
        full_ref, spread_sems = refs[0], refs[-1]
        refs = refs[1:-1]
    elif mode == HAND:
        next_ref, full_ref = refs[:2]
        hand_sems, spread_sems = refs[-2:]
        refs = refs[2:-2]
    (weight, total_ref, wsem, stat_send, stat_recv, ssem), refs = refs[:6], refs[6:]
    r = lax.axis_index(ROW)
    width = base_ref.shape[1]
    features = ROWS * width
    loads = load_blocks(pieces, weight, wsem, features, False)
    targets = [{ROW: peer_of(r, d)} for d in (1, 2, 3)]
    if mode == HAND:
        targets.append({GROUP: 1 - lax.axis_index(GROUP)})
    greet(targets, len(targets))
    for load in loads:
        load.wait()

    def partial(m, owner, cols):
        return sum(
            dot(grads[i][rows_of(m), :], weight[owner, i, cols, :], 1, 1) for i in range(n)
        )

    exchange = Exchange(r, refs)
    if mode == SPREAD:
        spread = Spread(r, full_ref, spread_sems)
    elif mode == HAND:
        hand = Hand(r, 1, out_ref, next_ref, full_ref, hand_sems, spread_sems)
    exchange.start(partial, total_ref)

    def stat_copy(m, d):
        return remote(
            stat_send.at[m],
            stat_recv.at[m, d - 1],
            ssem.at[0, m, d - 1],
            ssem.at[1, m, d - 1],
            {ROW: peer_of(r, d)},
        )

    gain = gain_ref[...]
    small = (jnp.zeros((1, width), F32), jnp.zeros((1, width), F32))

    def unit_at(at):
        return (base_ref[at, :].astype(BF16).astype(F32) - mean_ref[at, :]) * rstd_ref[at, :]

    for m in range(MICRO):
        exchange.wait(m)
        sums = []
        for here, at in row_steps(m):
            grad = total_ref[at, :] + exchange.received(m, here)
            total_ref[at, :] = grad
            unit = unit_at(at)
            product = grad * unit
            small = (
                small[0] + jnp.sum(product, axis=0, keepdims=True),
                small[1] + jnp.sum(grad, axis=0, keepdims=True),
            )
            first = jnp.sum(grad * gain, axis=-1, keepdims=True)
            second = jnp.sum(product * gain, axis=-1, keepdims=True)
            lane = lax.broadcasted_iota(jnp.int32, (here.stop - here.start, LANES), 1)
            sums.append(jnp.where(lane == 0, first, jnp.where(lane == 1, second, 0.0)))
        stat_send[m] = jnp.concatenate(sums, axis=0).T[0:8]
        for d in (3, 1, 2):
            stat_copy(m, d).start()
    small_ref[0:1, :] = small[0]
    small_ref[1:2, :] = small[1]

    for m in range(MICRO):
        sums = stat_send[m]
        for d in (1, 2, 3):
            stat_copy(m, d).wait()
            sums = sums + stat_recv[m, d - 1]
        sums = jnp.concatenate([sums, jnp.zeros((LANES - 8, TOK_DEV), F32)], axis=0).T
        for here, at in row_steps(m):
            own = sums[here]
            value = resid_ref[at, :].astype(F32) + rstd_ref[at, :] * (
                total_ref[at, :] * gain
                - own[:, 0:1] / features
                - unit_at(at) * (own[:, 1:2] / features)
            )
            out_ref[at, :] = value.astype(out_ref.dtype)
            if mode == SPREAD:
                full_ref[pl.ds(r, 1), at, :] = value.astype(BF16)[None]
        if mode == SPREAD:
            spread.start(m)
        elif mode == HAND:
            hand.start(m)
    if mode == SPREAD:
        for m in range(MICRO):
            spread.relay(m)
        for m in range(MICRO):
            spread.finish(m)
        spread.drain()
    elif mode == HAND:
        hand.finish()
    exchange.drain()


def back(grads, base, mean, rstd, gain, resid, pieces, mode):
    total, width = base.shape
    n = len(grads)
    out_shape = (
        jax.ShapeDtypeStruct((total, width), F32 if mode == SPREAD else BF16),
        jax.ShapeDtypeStruct((2, width), F32),
    )
    extra = []
    if mode == SPREAD:
        out_shape = out_shape + (jax.ShapeDtypeStruct((ROWS, total, width), BF16),)
        extra = [sems(*SPREAD_SEMS)]
    elif mode == HAND:
        out_shape = out_shape + hand_shapes(total, width)
        extra = list(HAND_SCRATCH)
    return pl.pallas_call(
        functools.partial(back_kernel, n, mode),
        out_shape=out_shape,
        in_specs=[VMEM] * (n + 5) + [HBM] * len(pieces),
        out_specs=(VMEM,) * len(out_shape),
        scratch_shapes=[
            pltpu.VMEM((ROWS, n, width, grads[0].shape[1]), BF16),
            pltpu.VMEM((total, width), F32),
            sems(len(pieces)),
            pltpu.VMEM((MICRO, 8, TOK_DEV), F32),
            pltpu.VMEM((MICRO, 3, 8, TOK_DEV), F32),
            sems(2, MICRO, 3),
        ]
        + exchange_scratch(width)
        + extra,
        compiler_params=comm_params((4, 5, 7)[mode]),
        cost_estimate=wire_estimate(30_000_000_000 if mode == SPREAD else 0),
    )(*grads, base, mean, rstd, gain, resid, *pieces)


def piece_block(ref, b, pieces):
    per_row = pieces // ROWS
    own = ref.shape[2] // per_row
    offset = pl.multiple_of(lax.rem(b, per_row) * own, own)
    return ref[b // per_row, :, pl.ds(offset, own)]


def rotate(chunk, cosine, near, far):
    return chunk * cosine + pltpu.roll(chunk, LANES - 8, 1) * near + pltpu.roll(chunk, 8, 1) * far


def attention_tiles():
    for i in range(TOK_DEV // LANES):
        yield slice(i * LANES, (i + 1) * LANES), (i + 1) * LANES


def head_masks(rows):
    lane = lax.broadcasted_iota(jnp.int32, (rows, LANES), 1)
    return lane < HEAD_DIM


def probabilities(query, keys, allowed, scaling):
    scores = dot(query, keys, 1, 1) * scaling
    scores = jnp.where(allowed > 0, scores, -1e30)
    totals = jnp.log(jnp.sum(jnp.exp(scores), axis=-1, keepdims=True))
    return jnp.exp(scores - totals)


def attention_kernel(
    scaling, full_ref, par_full_ref, rope_ref, allowed_ref, bias_ref, *refs
):
    pieces, refs = refs[:-7], refs[-7:]
    (normed_ref, mean_ref, rstd_ref, q_ref, k_ref, v_ref, att_ref) = refs
    pairs = len(pieces) // 2
    layer_norm(
        full_ref,
        normed_ref,
        mean_ref,
        rstd_ref,
        lambda b: par_full_ref[b, 0:1, :],
        lambda b: par_full_ref[b, 2:3, :],
        0,
        TOK_DEV,
    )
    blocks = [block_of(k, pairs) for k in range(len(pieces))]
    cosine, near, far = rope_ref[0, 0], rope_ref[0, 1], rope_ref[0, 2]
    for i, out_ref in enumerate((q_ref, k_ref, v_ref)):
        for start, size in tiles(out_ref.shape[1]):
            cols = slice(start, start + size)
            mixed = sum(
                dot(piece_block(normed_ref, b, len(pieces)), piece[i, :, cols], 1, 0)
                for b, piece in zip(blocks, pieces)
            )
            mixed = mixed + bias_ref[i : i + 1, cols]
            if i == 2:
                out_ref[:, cols] = mixed.astype(BF16)
                continue
            for part in range(0, size, LANES):
                chunk = rotate(mixed[:, part : part + LANES], cosine, near, far)
                out_ref[:, start + part : start + part + LANES] = chunk.astype(BF16)

    @pl.loop(0, q_ref.shape[1] // LANES)
    def _(h):
        cols = pl.ds(pl.multiple_of(h * LANES, LANES), LANES)
        for rows, count in attention_tiles():
            low = head_masks(LANES)
            query = q_ref[rows, cols]
            keys = k_ref[0:count, cols]
            values = v_ref[0:count, cols]
            allowed = allowed_ref[0, rows, 0:count]
            outs = []
            for mask in (low, ~low):
                probs = probabilities(
                    jnp.where(mask, query, jnp.zeros_like(query)), keys, allowed, scaling
                )
                outs.append(dot(probs.astype(BF16), values, 1, 0))
            att_ref[rows, cols] = jnp.where(low, outs[0], outs[1]).astype(BF16)


def constant(shape):
    return pl.BlockSpec(shape, lambda m: (0,) * len(shape), pipeline_mode=pl.Buffered(1))


def by_micro(shape, axis):
    return pl.BlockSpec(shape, lambda m: tuple(m if i == axis else 0 for i in range(len(shape))))


def estimate(flops, *arrays):
    total = sum(math.prod(a.shape) * a.dtype.itemsize for a in arrays)
    return pl.CostEstimate(flops=flops, bytes_accessed=total, transcendentals=0)


def attention(full, par_full, rope, allowed, bias, pieces):
    width = bias.shape[1]
    total = full.shape[1]
    out = jax.ShapeDtypeStruct((total, width), BF16)
    column = jax.ShapeDtypeStruct((total, 1), F32)
    block = by_micro((ROWS, TOK_DEV, full.shape[2]), 1)
    return pl.pallas_call(
        functools.partial(attention_kernel, 1.0 / math.sqrt(HEAD_DIM)),
        grid=(MICRO,),
        out_shape=(jax.ShapeDtypeStruct(full.shape, BF16), column, column) + (out,) * 4,
        in_specs=[
            block,
            constant(par_full.shape),
            by_micro((1,) + rope.shape[1:], 0),
            by_micro((1, TOK_DEV, TOK_DEV), 0),
            constant(bias.shape),
        ]
        + [constant(piece.shape) for piece in pieces],
        out_specs=(block,)
        + (by_micro((TOK_DEV, 1), 0),) * 2
        + (by_micro((TOK_DEV, width), 0),) * 4,
        cost_estimate=estimate(20 * total * ROWS * full.shape[2] * width, full, *pieces),
    )(full, par_full, rope, allowed, bias, *pieces)


def gate_up_kernel(normed_ref, *refs):
    pieces, (gate_ref, up_ref, act_ref) = refs[:-3], refs[-3:]
    pairs = len(pieces) // 2
    blocks = [block_of(k, pairs) for k in range(len(pieces))]
    for start, size in tiles(gate_ref.shape[1]):
        cols = slice(start, start + size)
        gate, up = [
            sum(
                dot(piece_block(normed_ref, b, len(pieces)), piece[i, :, cols], 1, 0)
                for b, piece in zip(blocks, pieces)
            )
            for i in range(2)
        ]
        gate_ref[:, cols] = gate
        up_ref[:, cols] = up
        act_ref[:, cols] = (gate / (1.0 + jnp.exp(-gate)) * up).astype(BF16)


def gate_up(normed, pieces):
    total, width = normed.shape[1], pieces[0].shape[2]
    return pl.pallas_call(
        gate_up_kernel,
        grid=(MICRO,),
        out_shape=(
            jax.ShapeDtypeStruct((total, width), F32),
            jax.ShapeDtypeStruct((total, width), F32),
            jax.ShapeDtypeStruct((total, width), BF16),
        ),
        in_specs=[by_micro((ROWS, TOK_DEV, normed.shape[2]), 1)]
        + [constant(piece.shape) for piece in pieces],
        out_specs=(by_micro((TOK_DEV, width), 0),) * 3,
        cost_estimate=estimate(4 * total * ROWS * normed.shape[2] * width, normed, *pieces),
    )(normed, *pieces)


def mlp_back_kernel(grad_ref, gate_ref, up_ref, *refs):
    pieces, (dgate_ref, dup_ref) = refs[:-2], refs[-2:]
    pairs = len(pieces) // 2
    blocks = [block_of(k, pairs) for k in range(len(pieces))]
    for start, size in tiles(gate_ref.shape[1]):
        cols = slice(start, start + size)
        grad = sum(
            dot(piece_block(grad_ref, b, len(pieces)), piece[cols, :], 1, 1)
            for b, piece in zip(blocks, pieces)
        )
        gate, up = gate_ref[:, cols], up_ref[:, cols]
        sigmoid = 1.0 / (1.0 + jnp.exp(-gate))
        dgate_ref[:, cols] = (grad * up * sigmoid * (1.0 + gate * (1.0 - sigmoid))).astype(BF16)
        dup_ref[:, cols] = (grad * (gate * sigmoid)).astype(BF16)


def mlp_back(grad_full, gate, up, pieces):
    total, width = gate.shape
    out = jax.ShapeDtypeStruct((total, width), BF16)
    return pl.pallas_call(
        mlp_back_kernel,
        grid=(MICRO,),
        out_shape=(out, out),
        in_specs=[
            by_micro((ROWS, TOK_DEV, grad_full.shape[2]), 1),
            by_micro((TOK_DEV, width), 0),
            by_micro((TOK_DEV, width), 0),
        ]
        + [constant(piece.shape) for piece in pieces],
        out_specs=(by_micro((TOK_DEV, width), 0),) * 2,
        cost_estimate=estimate(2 * total * ROWS * grad_full.shape[2] * width, gate, up, *pieces),
    )(grad_full, gate, up, *pieces)


def attention_back_kernel(
    scaling, grad_ref, q_ref, k_ref, v_ref, rope_ref, allowed_ref, *refs
):
    pieces, refs = refs[:-6], refs[-6:]
    (dq_ref, dk_ref, dv_ref, bias_ref, dk_sum, dv_sum) = refs
    pairs = len(pieces) // 2
    blocks = [block_of(k, pairs) for k in range(len(pieces))]
    for start, size in tiles(dq_ref.shape[1]):
        cols = slice(start, start + size)
        grad = sum(
            dot(piece_block(grad_ref, b, len(pieces)), piece[cols, :], 1, 1)
            for b, piece in zip(blocks, pieces)
        )
        dq_ref[:, cols] = grad.astype(BF16)
    cosine, near, far = rope_ref[0, 0], rope_ref[0, 1], rope_ref[0, 2]

    @pl.loop(0, q_ref.shape[1] // LANES)
    def _(h):
        cols = pl.ds(pl.multiple_of(h * LANES, LANES), LANES)
        dk_sum[...] = jnp.zeros_like(dk_sum)
        dv_sum[...] = jnp.zeros_like(dv_sum)
        bias = [jnp.zeros((1, LANES), F32) for _ in range(3)]
        for rows, count in attention_tiles():
            low = head_masks(LANES)
            query, grad = q_ref[rows, cols], dq_ref[rows, cols]
            keys, values = k_ref[0:count, cols], v_ref[0:count, cols]
            allowed = allowed_ref[0, rows, 0:count]
            dqs, dks, dvs = [], [], []
            for mask in (low, ~low):
                own_query = jnp.where(mask, query, jnp.zeros_like(query))
                own_grad = jnp.where(mask, grad, jnp.zeros_like(grad))
                probs = probabilities(own_query, keys, allowed, scaling)
                dprobs = dot(own_grad, values, 1, 1)
                inner = jnp.sum(probs * dprobs, axis=-1, keepdims=True)
                dscores = (probs * (dprobs - inner)).astype(BF16)
                dqs.append(dot(dscores, keys, 1, 0))
                dks.append(dot(dscores, own_query, 0, 0))
                dvs.append(dot(probs.astype(BF16), own_grad, 0, 0))
            dk_sum[0:count, :] += dks[0] + dks[1]
            dv_sum[0:count, :] += dvs[0] + dvs[1]
            dq = jnp.where(low, dqs[0], dqs[1]) * scaling
            dq = rotate(dq, cosine[rows], -near[rows], -far[rows]).astype(BF16)
            dq_ref[rows, cols] = dq
            bias[0] = bias[0] + jnp.sum(dq.astype(F32), axis=0, keepdims=True)
        dk = rotate(dk_sum[...] * scaling, cosine, -near, -far).astype(BF16)
        dk_ref[:, cols] = dk
        dv = dv_sum[...].astype(BF16)
        dv_ref[:, cols] = dv
        bias[1] = jnp.sum(dk.astype(F32), axis=0, keepdims=True)
        bias[2] = jnp.sum(dv.astype(F32), axis=0, keepdims=True)
        for i in range(3):
            bias_ref[0, i : i + 1, cols] = bias[i]


def attention_back(grad_full, queries, keys, values, rope, allowed, pieces):
    total, width = queries.shape
    out = jax.ShapeDtypeStruct((total, width), BF16)
    block = by_micro((TOK_DEV, width), 0)
    return pl.pallas_call(
        functools.partial(attention_back_kernel, 1.0 / math.sqrt(HEAD_DIM)),
        grid=(MICRO,),
        out_shape=(out, out, out, jax.ShapeDtypeStruct((MICRO, 3, width), F32)),
        in_specs=[
            by_micro((ROWS, TOK_DEV, grad_full.shape[2]), 1),
            block,
            block,
            block,
            by_micro((1,) + rope.shape[1:], 0),
            by_micro((1, TOK_DEV, TOK_DEV), 0),
        ]
        + [constant(piece.shape) for piece in pieces],
        out_specs=(block, block, block, by_micro((1, 3, width), 0)),
        scratch_shapes=[pltpu.VMEM((TOK_DEV, LANES), F32)] * 2,
        cost_estimate=estimate(4 * total * ROWS * grad_full.shape[2] * width, queries, *pieces),
    )(grad_full, queries, keys, values, rope, allowed, *pieces)


class ShardGrads:
    def __init__(self, plan, n, first, second, outs, scratch):
        count = len(plan)
        self.plan, self.n, self.first, self.second, self.outs = plan, n, first, second, outs
        self.loaded, scratch = scratch[:n], scratch[n:]
        self.gives, scratch = scratch[:count], scratch[count:]
        self.takes, scratch = scratch[:count], scratch[count:]
        self.turned, scratch = scratch[:count], scratch[count:]
        self.load_sems, self.move_sems = scratch
        self.pairs = self.gives[0].shape[0]
        self.partner = {SEC: 1 - lax.axis_index(SEC)}

    def load(self):
        for group, sources in enumerate((self.first, self.second)):

            @pl.when(lax.axis_index(GROUP) == group)
            def _(sources=sources):
                for i in range(self.n):
                    pltpu.make_async_copy(
                        sources[i], self.loaded[i], self.load_sems.at[i]
                    ).start()

    def move(self, w, j):
        return remote(
            self.gives[w].at[j],
            self.takes[w].at[j],
            self.move_sems.at[0, w, j],
            self.move_sems.at[1, w, j],
            self.partner,
        )

    def compute(self, w, k, store):
        left, rights, left_blocked = self.plan[w]
        loaded, turned = self.loaded, self.turned
        b = block_of(k, self.pairs)
        if left_blocked:
            turned[w][...] = piece_block(loaded[left], b, 2 * self.pairs).T
            for i, right in enumerate(rights):
                for start, size in tiles(loaded[right].shape[1]):
                    at = slice(start, start + size)
                    store(i, slice(None), at, dot(turned[w][...], loaded[right][:, at], 1, 0))
            return
        right = piece_block(loaded[rights[0]], b, 2 * self.pairs)
        for start, size in tiles(loaded[left].shape[1], 2 * WIDE):
            at = slice(start, start + size)
            store(0, at, slice(None), dot(turned[w][at, :], right, 1, 0))

    def run(self):
        for i in range(self.n):
            pltpu.make_async_copy(self.first[i], self.loaded[i], self.load_sems.at[i]).wait()
        for w, (left, _, left_blocked) in enumerate(self.plan):
            if not left_blocked:
                self.turned[w][...] = self.loaded[left][...].T
            for j in range(self.pairs):

                def give(i, rows, cols, value):
                    self.gives[w][j, i, rows, cols] = value.astype(BF16)

                self.compute(w, self.pairs + j, give)
                self.move(w, j).start()
        for w in range(len(self.plan)):
            for j in range(self.pairs):
                self.move(w, j).wait_recv()

                def keep(i, rows, cols, value):
                    total = value + self.takes[w][j, i, rows, cols].astype(F32)
                    if j == 0:
                        self.outs[2 * w][i, rows, cols] = total.astype(BF16)
                    else:
                        self.outs[2 * w + 1][j - 1, i, rows, cols] = total.astype(BF16)

                self.compute(w, j, keep)
        for w in range(len(self.plan)):
            for j in range(self.pairs):
                self.move(w, j).wait_send()


def shard_grads_kernel(plan, n, *refs):
    first, second, refs = refs[:n], refs[n : 2 * n], refs[2 * n :]
    count = 2 * len(plan)
    grads = ShardGrads(plan, n, first, second, refs[:count], refs[count:])
    grads.load()
    greet([grads.partner], 1)
    grads.run()


def shard_grads(plan, first, second, cols, collective_id):
    pairs = cols // 2
    n = len(first)
    total = first[plan[0][0]].shape[-2]
    out_shape, gives, turned, flops = [], [], [], 0
    for left, rights, left_blocked in plan:
        blocked = first[left] if left_blocked else first[rights[0]]
        own = ROWS * blocked.shape[2] // cols
        if left_blocked:
            shard = (len(rights), own, first[rights[0]].shape[1])
            turned.append(pltpu.VMEM((own, total), BF16))
        else:
            shard = (1, first[left].shape[1], own)
            turned.append(pltpu.VMEM((first[left].shape[1], total), BF16))
        out_shape.append(jax.ShapeDtypeStruct(shard, BF16))
        out_shape.append(jax.ShapeDtypeStruct((pairs - 1,) + shard, BF16))
        gives.append(pltpu.VMEM((pairs,) + shard, BF16))
        flops += 2 * cols * math.prod(shard) * total
    scratch = [pltpu.VMEM(a.shape, a.dtype) for a in first] + gives + gives + turned
    scratch += [sems(n), sems(2, len(plan), pairs)]
    outs = pl.pallas_call(
        functools.partial(shard_grads_kernel, plan, n),
        out_shape=out_shape,
        in_specs=[HBM] * (2 * n),
        out_specs=[VMEM] * len(out_shape),
        scratch_shapes=scratch,
        compiler_params=comm_params(collective_id),
        cost_estimate=estimate(2 * flops, *first, *out_shape),
    )(*first, *second)
    return list(zip(outs[0::2], outs[1::2]))


class Moves:
    def __init__(self):
        self.pairs = lax.axis_size(PAIR)
        self.cols = 2 * self.pairs
        self.s = lax.axis_index(SEC)
        self.g = lax.axis_index(GROUP)

    def send(self, value, moves):
        def flat(r, place):
            s, h, p = place
            return ((s * ROWS + r) * 2 + h) * self.pairs + p

        pairs = [(flat(r, a), flat(r, b)) for r in range(ROWS) for a, b in moves]
        return lax.ppermute(value, AXES, pairs)

    def places(self):
        return [(s, h, p) for s in range(2) for h in range(2) for p in range(self.pairs)]

    def swap(self, value):
        moves = [
            ((s, h, p), (s, h, p) if s == h else (h, s, p)) for s, h, p in self.places()
        ]
        return self.send(value, moves)

    def across(self, value):
        moves = [((s, h, p), (1 - s, h, p)) for s, h, p in self.places()]
        return self.send(value, moves)

    def along(self, value, j):
        moves = [((s, h, (p + j) % self.pairs), (s, h, p)) for s, h, p in self.places()]
        return self.send(value, moves)

    def back_along(self, value, j):
        moves = [((s, h, p), (s, h, (p + j) % self.pairs)) for s, h, p in self.places()]
        return self.send(value, moves)

    def homes(self):
        for g in range(2):
            for b in range(self.cols):
                yield (g, b // self.pairs, b % self.pairs), (b % 2, g, b // 2)

    def fetch_blocks(self, value):
        return self.send(value, list(self.homes()))

    def return_blocks(self, value):
        return self.send(value, [(b, a) for a, b in self.homes()])

    def alongs(self, near):
        return [near] + [self.along(near, j) for j in range(1, self.pairs)]

    def acrosses(self, near):
        return near + [self.across(shard) for shard in near]

    def total_small(self, value):
        value = value + self.across(value)
        total = value
        for j in range(1, self.pairs):
            total = total + self.along(value, j)
        return self.swap(total)

    def scatter_grads(self, own, rest):
        total = own.astype(F32)
        for j in range(1, self.pairs):
            total = total + self.back_along(rest[j - 1], j).astype(F32)
        return self.swap(total.astype(BF16))


def after(value, *earlier):
    return lax.optimization_barrier((value, *earlier))[0]


def layout(seq_lengths):
    end_points = jnp.cumsum(seq_lengths)
    places = jnp.arange(TOK_DEV, dtype=jnp.int32)
    passed = places[:, None] >= end_points[None, :]
    segment = jnp.sum(passed.astype(jnp.int32), axis=1)
    starts = jnp.sum(jnp.where(passed, seq_lengths[None, :], 0), axis=1)
    offset = (places - starts).astype(F32)
    allowed = (segment[:, None] == segment[None, :]) & (places[None, :] <= places[:, None])
    frequency = 10000.0 ** (-(jnp.arange(ROT // 2, dtype=F32) * 2.0 / ROT))
    angles = offset[:, None] * frequency[None, :]
    cosine, sine = jnp.cos(angles), jnp.sin(angles)
    rest = HEAD_DIM - ROT
    nothing = jnp.zeros_like(sine)
    tail = jnp.zeros((TOK_DEV, rest), F32)

    def lanes(*parts):
        head = jnp.concatenate(parts, axis=1)
        return jnp.concatenate([head, head], axis=1)

    rope = jnp.stack(
        [
            lanes(cosine, cosine, tail + 1.0),
            lanes(-sine, nothing, tail),
            lanes(nothing, sine, tail),
        ]
    )
    return allowed.astype(F32), rope


def on_device(
    inputs, lengths, norm_gain, norm_bias, w_qkv, b_qkv, w_out, w_gate_up, w_down, grad_out
):
    moves = Moves()
    width = inputs.shape[2]
    is_first = moves.g == 0

    own_lengths = moves.fetch_blocks(lengths)[:, 0]
    start = moves.fetch_blocks(jnp.where(moves.s == 0, inputs, grad_out))
    start = start.reshape(MICRO * TOK_DEV, width)
    par = jnp.concatenate([norm_gain[0], norm_bias[0], b_qkv[0], jnp.zeros((1, width), F32)])
    tables = [layout(own_lengths[m]) for m in range(MICRO)]
    allowed = jnp.stack([table[0] for table in tables])
    rope = jnp.stack([table[1] for table in tables])

    cols = moves.cols
    near_qkv = moves.swap(after(jnp.swapaxes(w_qkv[0], 0, 1), own_lengths))
    near_out = moves.swap(after(w_out[0], own_lengths))

    start_full, par_full, par = gather(start, par)
    shards_qkv = moves.acrosses(moves.alongs(after(near_qkv, par_full)))
    shards_out = moves.acrosses(moves.alongs(after(near_out, par_full)))
    near_gate_up = moves.swap(after(jnp.swapaxes(w_gate_up[0], 0, 1), par_full))

    def forward_one(full):
        normed, mean, rstd, *heads = attention(
            full, par_full, rope, allowed, par[4:7], shards_qkv
        )
        return (normed, mean, rstd), heads

    def forward_two(x, attended):
        hidden, _, normed, mean, rstd = out_norm(attended, x, par_full, shards_out)
        return hidden, normed, mean, rstd

    one_first, heads_first = forward_one(start_full)
    shards_gate_up = moves.acrosses(moves.alongs(near_gate_up))
    near_down = moves.swap(after(w_down[0], near_gate_up))
    two_first = forward_two(start, heads_first[3])
    shards_down = moves.acrosses(moves.alongs(after(near_down, one_first[1])))
    mlp_first = gate_up(two_first[1], shards_gate_up)
    out_first, x_second, full_second = down_and_hand(mlp_first[2], two_first[0], shards_down)

    one_second, heads_second = forward_one(full_second)
    two_second = forward_two(x_second, heads_second[3])
    mlp_second = gate_up(two_second[1], shards_gate_up)

    def backward_mlp(grad_full, mlp):
        return mlp_back(grad_full, mlp[0], mlp[1], shards_down)

    def backward_two(grad, dmlp, two):
        hidden, _, mean, rstd = two
        return back(dmlp, hidden, mean, rstd, par[1:2], grad, shards_gate_up, SPREAD)

    def backward_one(dhidden_full, heads):
        return attention_back(dhidden_full, *heads[:3], rope, allowed, shards_out)

    def backward_last(dheads, x, one, dhidden, mode):
        _, mean, rstd = one
        return back(dheads, x, mean, rstd, par[0:1], dhidden, shards_qkv, mode)

    dmlp_second = backward_mlp(start_full, mlp_second)
    dhidden_second, small_two_second, dhidden_full_second = backward_two(
        start, dmlp_second, two_second
    )
    *dheads_second, dbias_second = backward_one(dhidden_full_second, heads_second)
    grad_second, small_one_second, handed, handed_full = backward_last(
        dheads_second, x_second, one_second, dhidden_second, HAND
    )

    (sums_down,) = shard_grads(
        ((0, (1,), False),),
        (mlp_first[2], handed_full),
        (mlp_second[2], start_full),
        cols,
        8,
    )
    dmlp_first = backward_mlp(after(handed_full, sums_down[0]), mlp_first)
    (sums_gate_up,) = shard_grads(
        ((0, (1, 2), True),),
        (two_first[1], *dmlp_first),
        (two_second[1], *dmlp_second),
        cols,
        10,
    )
    early = moves.return_blocks(jnp.where(is_first, out_first, after(grad_second, sums_gate_up[0])))
    dhidden_first, small_two_first, dhidden_full_first = backward_two(
        handed, after(dmlp_first, sums_gate_up[0]), two_first
    )
    *dheads_first, dbias_first = backward_one(dhidden_full_first, heads_first)
    sums_qkv, sums_out = shard_grads(
        ((0, (1, 2, 3), True), (4, (5,), False)),
        (one_first[0], *dheads_first, heads_first[3], dhidden_full_first),
        (one_second[0], *dheads_second, heads_second[3], dhidden_full_second),
        cols,
        9,
    )
    grad_first, small_one_first = backward_last(
        after(dheads_first, sums_out[0]), start, one_first, dhidden_first, LAST
    )

    def pack(small_one, small_two, dbias):
        return jnp.concatenate(
            [
                small_one[0:1],
                small_two[0:1],
                small_one[1:2],
                small_two[1:2],
                jnp.sum(dbias, axis=0),
                jnp.zeros((1, width), F32),
            ]
        )

    sums = moves.total_small(
        jnp.where(
            is_first,
            pack(small_one_first, small_two_first, dbias_first),
            pack(small_one_second, small_two_second, dbias_second),
        )
    )
    parts = [moves.scatter_grads(*pair) for pair in (sums_qkv, sums_out, sums_gate_up, sums_down)]
    out_second = down_last(after(mlp_second[2], grad_first), two_second[0], shards_down)
    grad_gate_up = trade(parts[2])
    late = moves.return_blocks(jnp.where(is_first, grad_first, out_second))
    first_home = moves.s == 0
    activations = jnp.where(first_home, early, late)
    input_grad = jnp.where(first_home, late, early)
    return (
        activations.reshape(1, MICRO, TOK_DEV, width),
        input_grad.reshape(1, MICRO, TOK_DEV, width),
        sums[None, 0:2],
        sums[None, 2:4],
        jnp.swapaxes(parts[0].astype(F32), 0, 1)[None],
        sums[None, 4:7],
        parts[1].astype(F32),
        grad_gate_up[None],
        parts[3].astype(F32),
    )


def solution(mesh):
    cols = mesh.shape["col"]
    halves = Mesh(mesh.devices.reshape(2, mesh.shape[ROW], 2, cols // 2), AXES)
    rows, by_group, own_row = P(None, COL, ROW), P(SEC, None, COL, ROW), P(SEC, None, ROW)
    by_in, by_out = P(SEC, COL, None, ROW), P(SEC, ROW, COL)
    in_specs = (
        rows,
        P(None, COL, None),
        own_row,
        own_row,
        by_in,
        own_row,
        by_out,
        by_in,
        by_out,
        rows,
    )
    out_specs = (by_group, by_group, own_row, own_row, by_in, own_row, by_out, by_in, by_out)
    return jax.shard_map(
        on_device,
        mesh=halves,
        in_specs=in_specs,
        out_specs=out_specs,
        check_vma=False,
    )
```
